32 devices in a mesh: seq: 4 (over z), tp: 4 (over y, x), dp: 2 (over core).
Axes of the slice: x: 2, y: 2, z: 4, core: 2. Of those that a mesh axis runs over, the one named last changes fastest.
Arguments:
- x_ckpt: bfloat16 [1024, 5120], P(('dp', 'seq', 'tp')), parts along dimension 0, may hold values from -5 to 5
- bc_ckpt: bfloat16 [2, 1024, 128], P(None, ('dp', 'seq', 'tp')), parts along dimension 1, may hold values from -1 to 1
- step_sizes: float32 [80, 1024], P('tp', ('dp', 'seq')), parts along dimension 1, may hold values from 0.03 to 0.3
- decay_rate: float32 [80], P('tp'), may hold values from 0 to 1, as said below
- skip_gain: float32 [80], P('tp'), may hold values from 0.25 to 1.75
- grad_out: bfloat16 [1024, 5120], P(('dp', 'seq'), 'tp'), parts along dimension 0, may hold values from -3 to 3
Outputs:
- grad_x: bfloat16 [1024, 5120], P(('dp', 'seq'), 'tp'), parts along dimension 0
- grad_bc: float32 [2, 1024, 128], P(None, ('dp', 'seq', 'tp')), parts along dimension 1
- grad_step: float32 [80, 1024], P('tp', ('dp', 'seq')), parts along dimension 1
The draws below stay inside these ranges and needn't reach their ends.
There are 2 independent parts, one for each index of `dp`. The reference program is written for one: setup_inputs(seed, part) draws one part's arguments, and reference() takes and returns one part's arrays. A program takes and returns all parts, laid end to end along the dimension named above; an argument that names none is the same for every part. Nothing has to cross between parts.
Inputs may be any that keep to these rules, and one draw needn't show every extreme that they name: `decay_rate`: positive decay rates of the 80 heads.
All inputs are finite; a program needn't handle non-finite values.
Results may differ from the reference program's by a relative error of at most 0.001.
Values may be sent and summed in bfloat16 or wider, within the bound.
A program may use at most 128 MiB of HBM per device.

```python
import math
from functools import partial
import jax
import jax.numpy as jnp
from jax import lax

HEADS = 80
STATE = 128
BLOCK = 128
TOKENS = 512
INNER = 5120


def draw_decay_rate(key, part):
    rate_key = jax.random.fold_in(key, 11)
    top_rate = 0.5
    low_rate = 20.0 / TOKENS
    drawn = jax.random.uniform(rate_key, (HEADS,), minval=math.log(low_rate), maxval=math.log(top_rate))
    return jnp.exp(drawn).astype(jnp.float32)


def draw_step_sizes(key, part):
    level_key, factor_key = jax.random.split(jax.random.fold_in(key, 23))
    level = jnp.exp(jax.random.uniform(level_key, (HEADS, 1), minval=math.log(0.043), maxval=math.log(0.187)))
    factor = jnp.exp(jax.random.uniform(factor_key, (HEADS, TOKENS), minval=math.log(0.7), maxval=math.log(1.6)))
    return jnp.clip(level * factor, 0.03, 0.3).astype(jnp.float32)


def draw_bc_ckpt(key, part):
    sign_key, noise_key = jax.random.split(jax.random.fold_in(key, 37))
    direction = jnp.where(jax.random.bernoulli(sign_key, 0.5, (STATE,)), 1.0, -1.0)
    common = direction / (8.0 * math.sqrt(STATE))
    spread = 1.0 / math.sqrt(STATE)
    noise = jnp.clip(jax.random.normal(noise_key, (2, TOKENS, STATE)), -4.0, 4.0) * spread
    return jnp.clip(common[None, None, :] + noise, -1.0, 1.0).astype(jnp.bfloat16)


def draw_x_ckpt(key, part):
    offset_key, noise_key = jax.random.split(jax.random.fold_in(key, 41))
    offset = jnp.clip(0.8 * jax.random.normal(offset_key, (1, INNER)), -2.5, 2.5)
    noise = jnp.clip(0.6 * jax.random.normal(noise_key, (TOKENS, INNER)), -2.4, 2.4)
    return jnp.clip(offset + noise, -5.0, 5.0).astype(jnp.bfloat16)


def draw_grad_out(key, part):
    offset_key, noise_key = jax.random.split(jax.random.fold_in(key, 53))
    offset = jnp.clip(0.4 * jax.random.normal(offset_key, (1, INNER)), -1.5, 1.5)
    noise = jnp.clip(0.4 * jax.random.normal(noise_key, (TOKENS, INNER)), -1.5, 1.5)
    return jnp.clip(offset + noise, -3.0, 3.0).astype(jnp.bfloat16)


def setup_inputs(seed: int = 0, part: int = 0) -> dict:
    key_of = jax.random.split(jax.random.key(seed), 7)
    part_splits = jax.random.split(jax.random.fold_in(key_of[6], part), 7)
    return {
        "x_ckpt": draw_x_ckpt(jax.random.fold_in(jax.random.fold_in(key_of[6], part), 71), part),
        "bc_ckpt": draw_bc_ckpt(jax.random.fold_in(jax.random.fold_in(key_of[6], part), 71), part),
        "step_sizes": draw_step_sizes(jax.random.fold_in(jax.random.fold_in(key_of[6], part), 71), part),
        "decay_rate": draw_decay_rate(jax.random.fold_in(key_of[6], 71), part),
        "skip_gain": jnp.clip(1.0 + 0.15 * jax.random.normal(key_of[4], (HEADS,), jnp.float32), 0.25, 1.75),
        "grad_out": draw_grad_out(jax.random.fold_in(jax.random.fold_in(key_of[6], part), 71), part),
    }


highest = lax.Precision.HIGHEST

def block_step(head_rates, head_gains, carry_state, pieces):
    inputs, step_block, proj_b, proj_c = pieces
    head_count = step_block.shape[0]
    row_count = step_block.shape[1]
    values = inputs.astype(jnp.float32).reshape(row_count, head_count, -1)
    cumulative = jnp.cumsum(-head_rates[:, None] * step_block, axis=1)
    positions = jnp.arange(row_count, dtype=jnp.int32)
    causal = positions[:, None] >= positions[None, :]
    log_gaps = cumulative[:, :, None] - cumulative[:, None, :]
    within = jnp.where(causal, jnp.exp(jnp.where(causal, log_gaps, 0.0)), 0.0)
    scores = jnp.dot(proj_c, proj_b.T, precision=highest, preferred_element_type=jnp.float32)
    weights = within * scores[None, :, :] * step_block[:, None, :]
    local_part = jnp.einsum('hts,shp->thp', weights, values, precision=highest, preferred_element_type=jnp.float32)
    carried = jnp.einsum('tn,hpn->thp', proj_c, carry_state, precision=highest, preferred_element_type=jnp.float32)
    carried = carried * jnp.exp(cumulative).T[:, :, None]
    result = local_part + carried + head_gains[None, :, None] * values
    tail_weight = jnp.exp(cumulative[:, -1:] - cumulative) * step_block
    fresh_state = jnp.einsum('hs,shp,sn->hpn', tail_weight, values, proj_b, precision=highest, preferred_element_type=jnp.float32)
    final_state = jnp.exp(cumulative[:, -1])[:, None, None] * carry_state + fresh_state
    return (final_state, result.reshape(row_count, -1))

def run_blocks(inputs, step_sizes, proj_b, proj_c, start_state, head_rates, head_gains, block_rows):
    row_count = inputs.shape[0]
    block_count = row_count // block_rows
    head_count = step_sizes.shape[0]
    input_blocks = inputs.reshape(block_count, block_rows, inputs.shape[1])
    step_blocks = step_sizes.reshape(head_count, block_count, block_rows).transpose(1, 0, 2)
    b_blocks = proj_b.reshape(block_count, block_rows, proj_b.shape[1])
    c_blocks = proj_c.reshape(block_count, block_rows, proj_c.shape[1])
    stepper = jax.checkpoint(partial(block_step, head_rates, head_gains))
    final_state, results = lax.scan(stepper, start_state, (input_blocks, step_blocks, b_blocks, c_blocks))
    return (results.reshape(row_count, -1), final_state)

def reference(x_ckpt, bc_ckpt, step_sizes, decay_rate, skip_gain, grad_out):
    head_count = decay_rate.shape[0]
    head_width = x_ckpt.shape[1] // head_count
    proj_b = bc_ckpt[0].astype(jnp.float32)
    proj_c = bc_ckpt[1].astype(jnp.float32)
    start_state = jnp.zeros((head_count, head_width, proj_b.shape[1]), jnp.float32)

    def forward(inputs, basis_b, basis_c, step_block):
        output, final_state = run_blocks(inputs, step_block, basis_b, basis_c, start_state, decay_rate, skip_gain, BLOCK)
        return output
    output, pull_back = jax.vjp(forward, x_ckpt, proj_b, proj_c, step_sizes)
    grad_x, grad_b, grad_c, grad_step = pull_back(grad_out.astype(jnp.float32))
    return (grad_x, jnp.stack([grad_b, grad_c]), grad_step)
```

```python
import math
from functools import partial

import jax
import jax.numpy as jnp
from jax import lax
from jax.experimental import pallas as pl
from jax.experimental.pallas import tpu as pltpu
from jax.sharding import PartitionSpec as P

MESH = pl.DeviceIdType.MESH
F32 = jnp.float32
BF16 = jnp.bfloat16
HEAD_PAD = 32
SKEW = 4
SPAN = 125.0

NN = (((1,), (0,)), ((), ()))
NT = (((1,), (1,)), ((), ()))


def dot(a, b, dims=NN):
    return lax.dot_general(a, b, dims, preferred_element_type=F32)


def exact(a, b):
    return lax.dot_general(
        a, b, NN, precision=lax.Precision.HIGHEST, preferred_element_type=F32
    )


def split(v):
    high = v.astype(BF16)
    return high, (v - high.astype(F32)).astype(BF16)


def joined(a, b, dims=NN):
    return dot(jnp.concatenate(a, axis=1), jnp.concatenate(b, axis=dims[0][1][0]), dims)


def dot2(a, b, dims=NN):
    return joined((a, a), b, dims)


def dot2l(a, b, dims=NN):
    return joined(a, (b, b), dims)


def dot3(a, b, dims=NN):
    return joined((a[0], a[0], a[1]), (b[0], b[1], b[0]), dims)


def encode(v):
    top = jnp.max(jnp.abs(v), axis=0, keepdims=True)
    top = jnp.maximum(top, 1e-30)
    return jnp.exp2(v * (SPAN / top)).astype(BF16), top


def decode(code, top):
    return jnp.log(code.astype(F32)) * (top * (1.0 / (SPAN * math.log(2.0))))


def kernel(
    peers, blocks, head_width,
    x_ref, bc_ref, step_ref, rate_ref, gain_ref, dy_ref,
    gx_ref, gbc_ref, gstep_ref,
    x_in, dy_in, step_in, xr, bcr, part, rs,
    state_in, state_out, pull_in, fresh, pulled,
    code_fo, code_fi, code_bo, code_bi, top_fo, top_fi, top_bo, top_bi,
    xs_h, xs_l, ys_h, ys_l, xc, dyc, ec, ed, gain_row,
    stp, rates, gains, cums, mt_acc, bc_acc, dcum_acc, dir_acc, sm, bcm,
    send_x, recv_x, send_b, recv_b, own_sem,
    send_f, recv_f, send_g, recv_g, send_ft, recv_ft, send_gt, recv_gt, send_r, recv_r,
):
    me = lax.axis_index("tp")
    block = lax.axis_index("seq")
    head_count, tokens = step_ref.shape
    width = dy_ref.shape[1]
    rows = x_ref.shape[0]
    chunks, _, lanes = xc.shape
    chunk_heads = lanes // head_width
    groups = recv_x.shape[1]
    group_lanes = width // groups
    group_chunks = chunks // groups

    has_prev = block > 0
    has_next = block < blocks - 1

    own_bc = pltpu.make_async_copy(bc_ref, bcr.at[me], own_sem.at[0])
    load_x = pltpu.make_async_copy(x_ref, x_in, own_sem.at[1])
    own_x = pltpu.make_async_copy(
        x_ref.at[:, pl.ds(pl.multiple_of(me * width, 128), width)], xr.at[me], own_sem.at[2]
    )
    load_step = pltpu.make_async_copy(step_ref, step_in, own_sem.at[3])
    load_dy = pltpu.make_async_copy(dy_ref, dy_in, own_sem.at[4])
    own_bc.start()
    load_x.start()
    load_step.start()
    load_dy.start()
    own_x.start()

    barrier = pltpu.get_barrier_semaphore()
    for d in range(1, peers):
        pl.semaphore_signal(
            barrier, inc=1, device_id={"tp": lax.rem(me + d, peers)}, device_id_type=MESH
        )

    @pl.when(has_prev)
    def _():
        pl.semaphore_signal(barrier, inc=1, device_id={"seq": block - 1}, device_id_type=MESH)

    @pl.when(has_next)
    def _():
        pl.semaphore_signal(barrier, inc=1, device_id={"seq": block + 1}, device_id_type=MESH)

    def bc_copy(peer, slot):
        return pltpu.make_async_remote_copy(
            src_ref=bcr.at[me], dst_ref=bcr.at[slot],
            send_sem=send_b.at[peer], recv_sem=recv_b.at[slot],
            device_id={"tp": peer}, device_id_type=MESH,
        )

    def x_copy(peer, slot, g):
        start = pl.multiple_of(peer * width + g * group_lanes, 128)
        return pltpu.make_async_remote_copy(
            src_ref=x_in.at[:, pl.ds(start, group_lanes)],
            dst_ref=xr.at[slot, :, pl.ds(g * group_lanes, group_lanes)],
            send_sem=send_x.at[peer, g], recv_sem=recv_x.at[slot, g],
            device_id={"tp": peer}, device_id_type=MESH,
        )

    own_bc.wait()
    neighbours = jnp.where(has_prev, 1, 0) + jnp.where(has_next, 1, 0)
    pl.semaphore_wait(barrier, peers - 1 + neighbours)
    for d in range(1, peers):
        bc_copy(lax.rem(me + d, peers), me).start()
    load_x.wait()
    for g in range(groups):
        for d in range(1, peers):
            x_copy(lax.rem(me + d, peers), me, g).start()

    load_step.wait()
    stp[...] = jnp.zeros_like(stp)
    stp[0:head_count] = step_in[...]
    rates[...] = jnp.zeros_like(rates)
    gains[...] = jnp.zeros_like(gains)
    for h in range(head_count):
        rates[h : h + 1] = jnp.full((1, tokens), rate_ref[h], F32)
        gains[h : h + 1] = jnp.full((1, tokens), gain_ref[h], F32)
    row = lax.broadcasted_iota(jnp.int32, (tokens, tokens), 0)
    col = lax.broadcasted_iota(jnp.int32, (tokens, tokens), 1)
    upto = row <= col
    cum = exact(-rates[...] * stp[...], jnp.where(upto, 1.0, 0.0).astype(F32))
    cums[...] = cum
    stacked = jnp.concatenate(
        [jnp.exp(cum), jnp.exp(-cum) * stp[...], gains[...], jnp.zeros_like(cum)], axis=0
    )
    table = split(stacked.T)
    pick_row = lax.broadcasted_iota(jnp.int32, (4 * HEAD_PAD, lanes), 0)
    pick_head = lax.broadcasted_iota(jnp.int32, (4 * HEAD_PAD, lanes), 1) // head_width
    load_dy.wait()
    for c in range(chunks):
        def spread(q):
            hit = pick_row == (q * HEAD_PAD + c * chunk_heads) + pick_head
            return jnp.where(hit, 1.0, 0.0).astype(BF16)

        grown = dot2l(table, spread(0))
        ec[c] = grown
        ed[c] = dot2l(table, spread(1))
        gain_row[c] = dot2l((table[0][0:16], table[1][0:16]), spread(2))[0:8]
        dy = dy_in[:, c * lanes : (c + 1) * lanes]
        dyc[c] = dy
        high, low = split(grown * dy.astype(F32))
        ys_h[c] = high
        ys_l[c] = low

    def forward_copies(c):
        return (
            pltpu.make_async_remote_copy(
                src_ref=top_fo.at[c], dst_ref=top_fi.at[c],
                send_sem=send_ft.at[c], recv_sem=recv_ft.at[c],
                device_id={"seq": block + 1}, device_id_type=MESH,
            ),
            pltpu.make_async_remote_copy(
                src_ref=code_fo.at[c], dst_ref=code_fi.at[c],
                send_sem=send_f.at[c], recv_sem=recv_f.at[c],
                device_id={"seq": block + 1}, device_id_type=MESH,
            ),
        )

    def backward_copies(c):
        return (
            pltpu.make_async_remote_copy(
                src_ref=top_bo.at[c], dst_ref=top_bi.at[c],
                send_sem=send_gt.at[c], recv_sem=recv_gt.at[c],
                device_id={"seq": block - 1}, device_id_type=MESH,
            ),
            pltpu.make_async_remote_copy(
                src_ref=code_bo.at[c], dst_ref=code_bi.at[c],
                send_sem=send_g.at[c], recv_sem=recv_g.at[c],
                device_id={"seq": block - 1}, device_id_type=MESH,
            ),
        )

    def send_forward(c, value):
        code_fo[c], top_fo[c] = encode(value)
        for copy in forward_copies(c):
            copy.start()

    def send_backward(c, value):
        code_bo[c], top_bo[c] = encode(value)
        for copy in backward_copies(c):
            copy.start()

    def total_decay(c):
        return ec[c, tokens - 1 : tokens, :]

    for d in range(1, peers):
        source = lax.rem(me + d, peers)
        bc_copy(source, source).wait_recv()
    proj_b = bcr[:, 0].reshape(tokens, -1)
    proj_c = bcr[:, 1].reshape(tokens, -1)
    bcm[0] = proj_b
    bcm[1] = proj_c
    c_t = proj_c.astype(F32).T.astype(BF16)
    for c in range(chunks):
        pulled[c] = dot2(c_t, (ys_h[c], ys_l[c]))

        if c % group_chunks == group_chunks - 1:
            @pl.when(jnp.logical_and(jnp.logical_not(has_next), has_prev))
            def _():
                for k in range(c - group_chunks + 1, c + 1):
                    send_backward(k, pulled[k])

    b_t = proj_b.astype(F32).T.astype(BF16)
    scores_t = jnp.where(upto, dot(proj_b, proj_c, NT), 0.0)
    sm[0], sm[1] = split(scores_t)
    sm[2], sm[3] = split(scores_t.T)

    @pl.when(jnp.logical_not(has_prev))
    def _():
        state_in[...] = jnp.zeros_like(state_in)

    @pl.when(jnp.logical_not(has_next))
    def _():
        pull_in[...] = jnp.zeros_like(pull_in)

    mt_acc[...] = jnp.zeros_like(mt_acc)
    bc_acc[...] = jnp.zeros_like(bc_acc)
    dcum_acc[...] = jnp.zeros_like(dcum_acc)
    dir_acc[...] = jnp.zeros_like(dir_acc)

    own_x.wait()
    for g in range(groups):
        for d in range(1, peers):
            source = lax.rem(me + d, peers)
            x_copy(source, source, g).wait_recv()
        for c in range(g * group_chunks, (g + 1) * group_chunks):
            x = xr[:, :, c * lanes : (c + 1) * lanes].reshape(tokens, lanes)
            xc[c] = x
            pair = split(ed[c] * x.astype(F32))
            xs_h[c] = pair[0]
            xs_l[c] = pair[1]
            fresh[c] = dot2(b_t, pair)

        @pl.when(jnp.logical_not(has_prev))
        def _():
            for c in range(g * group_chunks, (g + 1) * group_chunks):
                state_out[c] = total_decay(c) * fresh[c]

            @pl.when(has_next)
            def _():
                for c in range(g * group_chunks, (g + 1) * group_chunks):
                    send_forward(c, state_out[c])

    def selector(c):
        head = lax.broadcasted_iota(jnp.int32, (HEAD_PAD, lanes), 0)
        of = lax.broadcasted_iota(jnp.int32, (HEAD_PAD, lanes), 1) // head_width
        return jnp.where(head == c * chunk_heads + of, 1.0, 0.0).astype(BF16)

    def step(s, carry):
        cf = s - SKEW * block
        cb = s - SKEW * (blocks - 1 - block)
        do_f = jnp.logical_and(cf >= 0, cf < chunks)
        do_b = jnp.logical_and(cb >= 0, cb < chunks)

        @pl.when(jnp.logical_and(do_f, has_prev))
        def _():
            for copy in forward_copies(cf):
                copy.wait_recv()
            entering = decode(code_fi[cf], top_fi[cf])
            state_in[cf] = entering
            leaving = total_decay(cf) * (entering + fresh[cf])
            state_out[cf] = leaving

            @pl.when(has_next)
            def _():
                send_forward(cf, leaving)

        @pl.when(jnp.logical_and(do_b, has_next))
        def _():
            for copy in backward_copies(cb):
                copy.wait_recv()
            arriving = decode(code_bi[cb], top_bi[cb])
            pull_in[cb] = arriving

            @pl.when(has_prev)
            def _():
                send_backward(cb, total_decay(cb) * arriving + pulled[cb])

        @pl.when(s < chunks)
        def _():
            xs = (xs_h[s], xs_l[s])
            ys = (ys_h[s], ys_l[s])
            mt_acc[...] += dot3(xs, ys, NT)

        @pl.when(do_f)
        def _():
            entering = split(state_in[cf])
            z = joined(
                (sm[2], sm[2], sm[3], bcm[1], bcm[1]),
                (xs_h[cf], xs_l[cf], xs_h[cf], *entering),
            )
            bc_acc[1] += dot3((ys_h[cf], ys_l[cf]), entering, NT)
            v = split(ec[cf] * dyc[cf].astype(F32) * z)
            dcum_acc[...] += dot2(selector(cf), v, NT)

        @pl.when(do_b)
        def _():
            leaving = split(total_decay(cb) * pull_in[cb])
            a2 = joined(
                (sm[0], sm[0], sm[1], bcm[0], bcm[0]),
                (ys_h[cb], ys_l[cb], ys_h[cb], *leaving),
            )
            bc_acc[0] += dot3((xs_h[cb], xs_l[cb]), leaving, NT)
            x = xc[cb].astype(F32)
            growth = ed[cb]
            gx = growth * a2 + gain_row[cb, 0:1, :] * dyc[cb].astype(F32)
            gx_ref[:, pl.ds(pl.multiple_of(cb * lanes, 128), lanes)] = gx.astype(BF16)
            direct = x * a2
            pick = selector(cb)
            dir_acc[...] += dot2(pick, split(direct), NT)
            dcum_acc[...] -= dot2(pick, split(growth * direct), NT)

        return carry

    lax.fori_loop(0, chunks + SKEW * (blocks - 1), step, 0)

    inner = jnp.where(upto, mt_acc[...], 0.0)
    grad_b = bc_acc[0] + dot2l(split(inner), bcm[1])
    grad_c = bc_acc[1] + dot2l(split(inner.T), bcm[0])
    for j in range(peers):
        part[j, 0] = grad_b[j * rows : (j + 1) * rows]
        part[j, 1] = grad_c[j * rows : (j + 1) * rows]

    def sum_copy(peer, slot):
        return pltpu.make_async_remote_copy(
            src_ref=part.at[peer], dst_ref=rs.at[slot],
            send_sem=send_r.at[peer], recv_sem=recv_r.at[slot],
            device_id={"tp": peer}, device_id_type=MESH,
        )

    for d in range(1, peers):
        sum_copy(lax.rem(me + d, peers), me).start()

    edge = jnp.zeros((HEAD_PAD, 8), F32)
    for c in range(chunks):
        both = (pull_in[c] * state_out[c]).reshape(-1, 8, lanes).sum(axis=0)
        edge = edge + dot2(selector(c), split(both), NT)
    edge = jnp.sum(edge, axis=1, keepdims=True)
    after = exact(dcum_acc[...], jnp.where(row >= col, 1.0, 0.0).astype(F32)) + edge
    gstep = jnp.exp(-cums[...]) * dir_acc[...] - rates[...] * after
    gstep_ref[...] = gstep[0:head_count]

    total = part[me]
    for d in range(1, peers):
        source = lax.rem(me + d, peers)
        sum_copy(source, source).wait_recv()
        total = total + rs[source]
    gbc_ref[...] = total

    for d in range(1, peers):
        peer = lax.rem(me + d, peers)
        bc_copy(peer, me).wait_send()
        for g in range(groups):
            x_copy(peer, me, g).wait_send()
        sum_copy(peer, me).wait_send()

    def drain(c, carry):
        @pl.when(has_next)
        def _():
            for copy in forward_copies(c):
                copy.wait_send()

        @pl.when(has_prev)
        def _():
            for copy in backward_copies(c):
                copy.wait_send()

        return carry

    lax.fori_loop(0, chunks, drain, 0)


def shards(x_ckpt, bc_ckpt, step_sizes, decay_rate, skip_gain, grad_out):
    peers, blocks = lax.axis_size("tp"), lax.axis_size("seq")
    rows = x_ckpt.shape[0]
    head_count, tokens = step_sizes.shape
    width = grad_out.shape[1]
    state = bc_ckpt.shape[2]
    lanes = 128
    chunks = width // lanes
    head_width = width // head_count
    groups = chunks // 2 if chunks % 2 == 0 else chunks
    wide = lambda dtype, size: pltpu.VMEM((chunks, size, lanes), dtype)
    dma = lambda n: pltpu.SemaphoreType.DMA((n,))
    vmem = pl.BlockSpec(memory_space=pltpu.VMEM)
    hbm = pl.BlockSpec(memory_space=pl.ANY)
    smem = pl.BlockSpec(memory_space=pltpu.SMEM)
    heads = pltpu.VMEM((HEAD_PAD, tokens), F32)
    return pl.pallas_call(
        partial(kernel, peers, blocks, head_width),
        out_shape=(
            pltpu.VMEM((tokens, width), BF16),
            pltpu.VMEM((2, rows, state), F32),
            pltpu.VMEM((head_count, tokens), F32),
        ),
        in_specs=[hbm, hbm, hbm, smem, smem, hbm],
        out_specs=(vmem, vmem, vmem),
        scratch_shapes=[
            pltpu.VMEM(x_ckpt.shape, BF16),
            pltpu.VMEM((tokens, width), BF16),
            pltpu.VMEM((head_count, tokens), F32),
            pltpu.VMEM((peers, rows, width), BF16),
            pltpu.VMEM((peers, 2, rows, state), BF16),
            pltpu.VMEM((peers, 2, rows, state), F32),
            pltpu.VMEM((peers, 2, rows, state), F32),
            *[wide(F32, state)] * 5,
            *[wide(BF16, state)] * 4,
            *[wide(F32, 1)] * 4,
            *[wide(BF16, tokens)] * 6,
            *[wide(F32, tokens)] * 2,
            wide(F32, 8),
            heads, heads, heads, heads,
            pltpu.VMEM((tokens, tokens), F32),
            pltpu.VMEM((2, tokens, state), F32),
            heads, heads,
            pltpu.VMEM((4, tokens, tokens), BF16),
            pltpu.VMEM((2, tokens, state), BF16),
            pltpu.SemaphoreType.DMA((peers, groups)), pltpu.SemaphoreType.DMA((peers, groups)),
            dma(peers), dma(peers), dma(5),
            *[dma(chunks)] * 8,
            dma(peers), dma(peers),
        ],
        compiler_params=pltpu.CompilerParams(collective_id=0, has_side_effects=True),
    )(x_ckpt, bc_ckpt, step_sizes, decay_rate, skip_gain, grad_out)


def solution(mesh):
    return jax.shard_map(
        shards,
        mesh=mesh,
        in_specs=(
            P(("dp", "seq", "tp"), None),
            P(None, ("dp", "seq", "tp"), None),
            P("tp", ("dp", "seq")),
            P("tp"),
            P("tp"),
            P(("dp", "seq"), "tp"),
        ),
        out_specs=(
            P(("dp", "seq"), "tp"),
            P(None, ("dp", "seq", "tp"), None),
            P("tp", ("dp", "seq")),
        ),
        check_vma=False,
    )
```

```python
import math
from functools import partial

import jax
import jax.numpy as jnp
from jax import lax
from jax.experimental import pallas as pl
from jax.experimental.pallas import tpu as pltpu
from jax.sharding import PartitionSpec as P

MESH = pl.DeviceIdType.MESH
F32 = jnp.float32
BF16 = jnp.bfloat16
HEAD_PAD = 32
SKEW = 4
SPAN = 125.0
TOP_ROWS = 8

NN = (((1,), (0,)), ((), ()))
NT = (((1,), (1,)), ((), ()))


def dot(a, b, dims=NN):
    return lax.dot_general(a, b, dims, preferred_element_type=F32)


def exact(a, b):
    return lax.dot_general(
        a, b, NN, precision=lax.Precision.HIGHEST, preferred_element_type=F32
    )


def split(v):
    high = v.astype(BF16)
    return high, (v - high.astype(F32)).astype(BF16)


def joined(a, b, dims=NN):
    return dot(jnp.concatenate(a, axis=1), jnp.concatenate(b, axis=dims[0][1][0]), dims)


def dot2(a, b, dims=NN):
    return joined((a, a), b, dims)


def dot2l(a, b, dims=NN):
    return joined(a, (b, b), dims)


def dot3(a, b, dims=NN):
    return joined((a[0], a[0], a[1]), (b[0], b[1], b[0]), dims)


def encode(v):
    top = jnp.max(jnp.abs(v), axis=0, keepdims=True)
    top = jnp.maximum(top, 1e-30).astype(BF16)
    code = jnp.exp2(v * (SPAN / top.astype(F32))).astype(BF16)
    return jnp.concatenate([code, jnp.broadcast_to(top, (TOP_ROWS, v.shape[1]))], axis=0)


def decode(message):
    size = message.shape[0] - TOP_ROWS
    top = message[size : size + 1].astype(F32)
    return jnp.log(message[0:size].astype(F32)) * (top * (1.0 / (SPAN * math.log(2.0))))


def kernel(
    peers, blocks, head_width,
    x_ref, bc_ref, step_ref, rate_ref, gain_ref, dy_ref,
    gx_ref, gbc_ref, gstep_ref,
    x_in, dy_in, step_in, xr, bcr, rs,
    state_in, state_out, pull_in, fresh, pulled,
    code_fo, code_fi, code_bo, code_bi,
    xs_h, xs_l, ys_h, ys_l, xc, dyc, ec, ed, gain_row,
    stp, rates, gains, cums, bc_acc, dcum_acc, dir_acc, sm, bcm,
    rate_sm, gain_sm, own_sem, send_sem, recv_x, recv_b, recv_f, recv_g, recv_r,
):
    me = lax.axis_index("tp")
    block = lax.axis_index("seq")
    head_count, tokens = step_ref.shape
    width = dy_ref.shape[1]
    rows = x_ref.shape[0]
    chunks, _, lanes = xc.shape
    chunk_heads = lanes // head_width
    groups = recv_x.shape[0]
    group_lanes = width // groups
    group_chunks = chunks // groups

    has_prev = block > 0
    has_next = block < blocks - 1

    barrier = pltpu.get_barrier_semaphore()
    for d in range(1, peers):
        pl.semaphore_signal(
            barrier, inc=1, device_id={"tp": lax.rem(me + d, peers)}, device_id_type=MESH
        )

    @pl.when(has_prev)
    def _():
        pl.semaphore_signal(barrier, inc=1, device_id={"seq": block - 1}, device_id_type=MESH)

    @pl.when(has_next)
    def _():
        pl.semaphore_signal(barrier, inc=1, device_id={"seq": block + 1}, device_id_type=MESH)

    own_bc = pltpu.make_async_copy(bc_ref, bcr.at[me], own_sem.at[0])
    load_x = pltpu.make_async_copy(x_ref, x_in, own_sem.at[1])
    own_x = pltpu.make_async_copy(
        x_ref.at[:, pl.ds(pl.multiple_of(me * width, 128), width)], xr.at[me], own_sem.at[2]
    )
    load_step = pltpu.make_async_copy(step_ref, step_in, own_sem.at[3])
    load_dy = pltpu.make_async_copy(dy_ref, dy_in, own_sem.at[4])
    load_rate = pltpu.make_async_copy(rate_ref, rate_sm, own_sem.at[5])
    load_gain = pltpu.make_async_copy(gain_ref, gain_sm, own_sem.at[6])
    own_bc.start()
    load_x.start()
    load_step.start()
    load_dy.start()
    own_x.start()
    load_rate.start()
    load_gain.start()

    def bc_copy(peer, slot):
        return pltpu.make_async_remote_copy(
            src_ref=bcr.at[me], dst_ref=bcr.at[slot],
            send_sem=send_sem.at[0], recv_sem=recv_b.at[0],
            device_id={"tp": peer}, device_id_type=MESH,
        )

    def x_copy(peer, slot, g):
        start = pl.multiple_of(peer * width + g * group_lanes, 128)
        return pltpu.make_async_remote_copy(
            src_ref=x_in.at[:, pl.ds(start, group_lanes)],
            dst_ref=xr.at[slot, :, pl.ds(g * group_lanes, group_lanes)],
            send_sem=send_sem.at[1], recv_sem=recv_x.at[g],
            device_id={"tp": peer}, device_id_type=MESH,
        )

    own_bc.wait()
    neighbours = jnp.where(has_prev, 1, 0) + jnp.where(has_next, 1, 0)
    pl.semaphore_wait(barrier, peers - 1 + neighbours)
    for d in range(1, peers):
        bc_copy(lax.rem(me + d, peers), me).start()
    load_x.wait()
    for g in range(groups):
        for d in range(1, peers):
            x_copy(lax.rem(me + d, peers), me, g).start()

    load_step.wait()
    load_rate.wait()
    load_gain.wait()
    stp[...] = jnp.zeros_like(stp)
    stp[0:head_count] = step_in[...]
    rates[...] = jnp.zeros_like(rates)
    gains[...] = jnp.zeros_like(gains)
    for h in range(head_count):
        rates[h : h + 1] = jnp.full((1, tokens), rate_sm[h], F32)
        gains[h : h + 1] = jnp.full((1, tokens), gain_sm[h], F32)
    row = lax.broadcasted_iota(jnp.int32, (tokens, tokens), 0)
    col = lax.broadcasted_iota(jnp.int32, (tokens, tokens), 1)
    upto = row <= col
    cum = exact(-rates[...] * stp[...], jnp.where(upto, 1.0, 0.0).astype(F32))
    cums[...] = cum
    stacked = jnp.concatenate(
        [jnp.exp(cum), jnp.exp(-cum) * stp[...], gains[...], jnp.zeros_like(cum)], axis=0
    )
    table = split(stacked.T)
    pick_row = lax.broadcasted_iota(jnp.int32, (4 * HEAD_PAD, lanes), 0)
    pick_head = lax.broadcasted_iota(jnp.int32, (4 * HEAD_PAD, lanes), 1) // head_width
    load_dy.wait()
    for c in range(chunks):
        def spread(q):
            hit = pick_row == (q * HEAD_PAD + c * chunk_heads) + pick_head
            return jnp.where(hit, 1.0, 0.0).astype(BF16)

        grown = dot2l(table, spread(0))
        ec[c] = grown
        ed[c] = dot2l(table, spread(1))
        gain_row[c] = dot2l((table[0][0:16], table[1][0:16]), spread(2))[0:8]
        dy = dy_in[:, c * lanes : (c + 1) * lanes]
        dyc[c] = dy
        high, low = split(grown * dy.astype(F32))
        ys_h[c] = high
        ys_l[c] = low

    def forward_copy(c):
        return pltpu.make_async_remote_copy(
            src_ref=code_fo.at[c], dst_ref=code_fi.at[c],
            send_sem=send_sem.at[2], recv_sem=recv_f.at[c],
            device_id={"seq": block + 1}, device_id_type=MESH,
        )

    def backward_copy(c):
        return pltpu.make_async_remote_copy(
            src_ref=code_bo.at[c], dst_ref=code_bi.at[c],
            send_sem=send_sem.at[3], recv_sem=recv_g.at[c],
            device_id={"seq": block - 1}, device_id_type=MESH,
        )

    def landing(ref, sem, slot):
        return pltpu.make_async_remote_copy(
            src_ref=ref, dst_ref=ref, send_sem=send_sem.at[slot], recv_sem=sem,
            device_id={"tp": lax.rem(me + 1, peers)}, device_id_type=MESH,
        )

    def send_forward(c, value):
        code_fo[c] = encode(value)
        forward_copy(c).start()

    def send_backward(c, value):
        code_bo[c] = encode(value)
        backward_copy(c).start()

    def total_decay(c):
        return ec[c, tokens - 1 : tokens, :]

    landing(bcr.at[pl.ds(0, peers - 1)], recv_b.at[0], 0).wait_recv()
    proj_b = bcr[:, 0].reshape(tokens, -1)
    proj_c = bcr[:, 1].reshape(tokens, -1)
    bcm[0] = proj_b
    bcm[1] = proj_c
    c_t = proj_c.astype(F32).T.astype(BF16)
    for c in range(chunks):
        pulled[c] = dot2(c_t, (ys_h[c], ys_l[c]))

        if c % group_chunks == group_chunks - 1:
            @pl.when(jnp.logical_and(jnp.logical_not(has_next), has_prev))
            def _():
                for k in range(c - group_chunks + 1, c + 1):
                    send_backward(k, pulled[k])

    b_t = proj_b.astype(F32).T.astype(BF16)
    scores_t = jnp.where(upto, dot(proj_b, proj_c, NT), 0.0)
    sm[0], sm[1] = split(scores_t)
    sm[2], sm[3] = split(scores_t.T)

    @pl.when(jnp.logical_not(has_prev))
    def _():
        state_in[...] = jnp.zeros_like(state_in)

    @pl.when(jnp.logical_not(has_next))
    def _():
        pull_in[...] = jnp.zeros_like(pull_in)

    dcum_acc[...] = jnp.zeros_like(dcum_acc)
    dir_acc[...] = jnp.zeros_like(dir_acc)

    own_x.wait()
    for g in range(groups):
        group = xr.at[pl.ds(0, peers - 1), :, pl.ds(g * group_lanes, group_lanes)]
        landing(group, recv_x.at[g], 1).wait_recv()
        for c in range(g * group_chunks, (g + 1) * group_chunks):
            x = xr[:, :, c * lanes : (c + 1) * lanes].reshape(tokens, lanes)
            xc[c] = x
            pair = split(ed[c] * x.astype(F32))
            xs_h[c] = pair[0]
            xs_l[c] = pair[1]
            fresh[c] = dot2(b_t, pair)

        @pl.when(jnp.logical_not(has_prev))
        def _():
            for c in range(g * group_chunks, (g + 1) * group_chunks):
                state_out[c] = total_decay(c) * fresh[c]

            @pl.when(has_next)
            def _():
                for c in range(g * group_chunks, (g + 1) * group_chunks):
                    send_forward(c, state_out[c])

    inner = jnp.zeros((tokens, tokens), F32)
    for c in range(chunks):
        inner += dot3((xs_h[c], xs_l[c]), (ys_h[c], ys_l[c]), NT)
    inner = jnp.where(upto, inner, 0.0)
    bc_acc[0] = dot2l(split(inner), bcm[1])
    bc_acc[1] = dot2l(split(inner.T), bcm[0])

    def sum_copy(q, peer, slot):
        return pltpu.make_async_remote_copy(
            src_ref=bc_acc.at[q, pl.ds(pl.multiple_of(peer * rows, 8), rows)],
            dst_ref=rs.at[q, slot],
            send_sem=send_sem.at[4 + q], recv_sem=recv_r.at[q],
            device_id={"tp": peer}, device_id_type=MESH,
        )

    def send_sums(q):
        for d in range(1, peers):
            sum_copy(q, lax.rem(me + d, peers), me).start()

    @pl.when(jnp.logical_not(has_prev))
    def _():
        send_sums(1)

    @pl.when(jnp.logical_not(has_next))
    def _():
        send_sums(0)

    def selector(c):
        head = lax.broadcasted_iota(jnp.int32, (HEAD_PAD, lanes), 0)
        of = lax.broadcasted_iota(jnp.int32, (HEAD_PAD, lanes), 1) // head_width
        return jnp.where(head == c * chunk_heads + of, 1.0, 0.0).astype(BF16)

    def step(s, carry):
        cf = s - SKEW * block
        cb = s - SKEW * (blocks - 1 - block)
        do_f = jnp.logical_and(cf >= 0, cf < chunks)
        do_b = jnp.logical_and(cb >= 0, cb < chunks)

        @pl.when(jnp.logical_and(do_f, has_prev))
        def _():
            forward_copy(cf).wait_recv()
            entering = decode(code_fi[cf])
            state_in[cf] = entering
            leaving = total_decay(cf) * (entering + fresh[cf])
            state_out[cf] = leaving

            @pl.when(has_next)
            def _():
                send_forward(cf, leaving)

        @pl.when(jnp.logical_and(do_b, has_next))
        def _():
            backward_copy(cb).wait_recv()
            arriving = decode(code_bi[cb])
            pull_in[cb] = arriving

            @pl.when(has_prev)
            def _():
                send_backward(cb, total_decay(cb) * arriving + pulled[cb])

        @pl.when(do_f)
        def _():
            entering = split(state_in[cf])
            z = joined(
                (sm[2], sm[2], sm[3], bcm[1], bcm[1]),
                (xs_h[cf], xs_l[cf], xs_h[cf], *entering),
            )

            @pl.when(has_prev)
            def _():
                bc_acc[1] += dot3((ys_h[cf], ys_l[cf]), entering, NT)

            v = split(ec[cf] * dyc[cf].astype(F32) * z)
            dcum_acc[...] += dot2(selector(cf), v, NT)

        @pl.when(do_b)
        def _():
            leaving = split(total_decay(cb) * pull_in[cb])
            a2 = joined(
                (sm[0], sm[0], sm[1], bcm[0], bcm[0]),
                (ys_h[cb], ys_l[cb], ys_h[cb], *leaving),
            )

            @pl.when(has_next)
            def _():
                bc_acc[0] += dot3((xs_h[cb], xs_l[cb]), leaving, NT)

            x = xc[cb].astype(F32)
            growth = ed[cb]
            gx = growth * a2 + gain_row[cb, 0:1, :] * dyc[cb].astype(F32)
            gx_ref[:, pl.ds(pl.multiple_of(cb * lanes, 128), lanes)] = gx.astype(BF16)
            direct = x * a2
            pick = selector(cb)
            dir_acc[...] += dot2(pick, split(direct), NT)
            dcum_acc[...] -= dot2(pick, split(growth * direct), NT)

        return carry

    lax.fori_loop(0, chunks + SKEW * (blocks - 1), step, 0)

    @pl.when(has_prev)
    def _():
        send_sums(1)

    @pl.when(has_next)
    def _():
        send_sums(0)

    edge = jnp.zeros((HEAD_PAD, 8), F32)
    for c in range(chunks):
        both = (pull_in[c] * state_out[c]).reshape(-1, 8, lanes).sum(axis=0)
        edge = edge + dot2(selector(c), split(both), NT)
    edge = jnp.sum(edge, axis=1, keepdims=True)
    after = exact(dcum_acc[...], jnp.where(row >= col, 1.0, 0.0).astype(F32)) + edge
    gstep = jnp.exp(-cums[...]) * dir_acc[...] - rates[...] * after
    gstep_ref[...] = gstep[0:head_count]

    for q in range(2):
        landing(rs.at[q, pl.ds(0, peers - 1)], recv_r.at[q], 4 + q).wait_recv()
        total = bc_acc[q, pl.ds(pl.multiple_of(me * rows, 8), rows)]
        for d in range(1, peers):
            total = total + rs[q, lax.rem(me + d, peers)]
        gbc_ref[q] = total

    landing(bcr.at[pl.ds(0, peers - 1)], recv_b.at[0], 0).wait_send()
    landing(xr.at[pl.ds(0, peers - 1)], recv_x.at[0], 1).wait_send()
    for q in range(2):
        landing(rs.at[q, pl.ds(0, peers - 1)], recv_r.at[q], 4 + q).wait_send()

    @pl.when(has_next)
    def _():
        landing(code_fo, recv_f.at[0], 2).wait_send()

    @pl.when(has_prev)
    def _():
        landing(code_bo, recv_g.at[0], 3).wait_send()


def store(gx_ref, gbc_ref, gstep_ref, gx_out, gbc_out, gstep_out, sems):
    copies = [
        pltpu.make_async_copy(source, target, sems.at[k])
        for k, (source, target) in enumerate(
            ((gx_ref, gx_out), (gbc_ref, gbc_out), (gstep_ref, gstep_out))
        )
    ]
    for copy in copies:
        copy.start()
    for copy in copies:
        copy.wait()


def shards(x_ckpt, bc_ckpt, step_sizes, decay_rate, skip_gain, grad_out):
    peers, blocks = lax.axis_size("tp"), lax.axis_size("seq")
    rows = x_ckpt.shape[0]
    head_count, tokens = step_sizes.shape
    width = grad_out.shape[1]
    state = bc_ckpt.shape[2]
    lanes = 128
    chunks = width // lanes
    head_width = width // head_count
    groups = chunks // 2 if chunks % 2 == 0 else chunks
    wide = lambda dtype, size: pltpu.VMEM((chunks, size, lanes), dtype)
    dma = lambda n: pltpu.SemaphoreType.DMA((n,))
    vmem = pl.BlockSpec(memory_space=pltpu.VMEM)
    hbm = pl.BlockSpec(memory_space=pl.ANY)
    heads = pltpu.VMEM((HEAD_PAD, tokens), F32)
    outs = (
        ((tokens, width), BF16),
        ((2, rows, state), F32),
        ((head_count, tokens), F32),
    )
    grads = pl.pallas_call(
        partial(kernel, peers, blocks, head_width),
        out_shape=tuple(pltpu.VMEM(shape, dtype) for shape, dtype in outs),
        in_specs=[hbm] * 6,
        out_specs=(vmem, vmem, vmem),
        scratch_shapes=[
            pltpu.VMEM(x_ckpt.shape, BF16),
            pltpu.VMEM((tokens, width), BF16),
            pltpu.VMEM((head_count, tokens), F32),
            pltpu.VMEM((peers, rows, width), BF16),
            pltpu.VMEM((peers, 2, rows, state), BF16),
            pltpu.VMEM((2, peers, rows, state), F32),
            *[wide(F32, state)] * 5,
            *[wide(BF16, state + TOP_ROWS)] * 4,
            *[wide(BF16, tokens)] * 6,
            *[wide(F32, tokens)] * 2,
            wide(F32, 8),
            heads, heads, heads, heads,
            pltpu.VMEM((2, tokens, state), F32),
            heads, heads,
            pltpu.VMEM((4, tokens, tokens), BF16),
            pltpu.VMEM((2, tokens, state), BF16),
            pltpu.SMEM((head_count,), F32), pltpu.SMEM((head_count,), F32),
            dma(7), dma(6), dma(groups), dma(1), dma(chunks), dma(chunks), dma(2),
        ],
        compiler_params=pltpu.CompilerParams(collective_id=0, has_side_effects=True),
    )(x_ckpt, bc_ckpt, step_sizes, decay_rate, skip_gain, grad_out)
    return pl.pallas_call(
        store,
        out_shape=tuple(jax.ShapeDtypeStruct(shape, dtype) for shape, dtype in outs),
        in_specs=[vmem] * 3,
        out_specs=(hbm,) * 3,
        scratch_shapes=[dma(3)],
    )(*[pltpu.with_memory_space_constraint(grad, pltpu.VMEM) for grad in grads])


def solution(mesh):
    return jax.shard_map(
        shards,
        mesh=mesh,
        in_specs=(
            P(("dp", "seq", "tp"), None),
            P(None, ("dp", "seq", "tp"), None),
            P("tp", ("dp", "seq")),
            P("tp"),
            P("tp"),
            P(("dp", "seq"), "tp"),
        ),
        out_specs=(
            P(("dp", "seq"), "tp"),
            P(None, ("dp", "seq", "tp"), None),
            P("tp", ("dp", "seq")),
        ),
        check_vma=False,
    )
```

```python
import math
from functools import partial

import jax
import jax.numpy as jnp
from jax import lax
from jax.experimental import pallas as pl
from jax.experimental.pallas import tpu as pltpu
from jax.sharding import PartitionSpec as P

MESH = pl.DeviceIdType.MESH
F32 = jnp.float32
BF16 = jnp.bfloat16
HEAD_PAD = 32
SKEW = 4
LAG = 2
EARLY = 2
SPAN = 125.0
TOP_ROWS = 8

NN = (((1,), (0,)), ((), ()))
NT = (((1,), (1,)), ((), ()))


def dot(a, b, dims=NN):
    return lax.dot_general(a, b, dims, preferred_element_type=F32)


def exact(a, b):
    return lax.dot_general(
        a, b, NN, precision=lax.Precision.HIGHEST, preferred_element_type=F32
    )


def split(v):
    high = v.astype(BF16)
    return high, (v - high.astype(F32)).astype(BF16)


def joined(a, b, dims=NN):
    return dot(jnp.concatenate(a, axis=1), jnp.concatenate(b, axis=dims[0][1][0]), dims)


def dot2(a, b, dims=NN):
    return joined((a, a), b, dims)


def dot2l(a, b, dims=NN):
    return joined(a, (b, b), dims)


def dot3(a, b, dims=NN):
    return joined((a[0], a[0], a[1]), (b[0], b[1], b[0]), dims)


def encode(v):
    top = jnp.max(jnp.abs(v), axis=0, keepdims=True)
    top = jnp.maximum(top, 1e-30).astype(BF16)
    code = jnp.exp2(v * (SPAN / top.astype(F32))).astype(BF16)
    return jnp.concatenate([code, jnp.broadcast_to(top, (TOP_ROWS, v.shape[1]))], axis=0)


def decode(message):
    size = message.shape[0] - TOP_ROWS
    top = message[size : size + 1].astype(F32)
    return jnp.log(message[0:size].astype(F32)) * (top * (1.0 / (SPAN * math.log(2.0))))


def kernel(
    peers, blocks, head_width,
    x_ref, bc_ref, step_ref, rate_ref, gain_ref, dy_ref,
    gx_ref, gbc_ref, gstep_ref,
    x_in, dy_in, step_in, xr, bcr, rs,
    state_in, state_out, pull_in, fresh, pulled,
    code_fo, code_fi, code_bo, code_bi,
    near_x, near_b, near_step, next_dy, next_c, next_step, pads, weights, sides,
    xs_h, xs_l, ys_h, ys_l, xc, dyc, ec, ed, gain_row,
    stp, rates, gains, cums, bc_acc, dcum_acc, dir_acc, sm, bcm,
    rate_sm, gain_sm, own_sem, send_sem, recv_x, recv_b, recv_f, recv_g, recv_r, recv_n,
):
    me = lax.axis_index("tp")
    block = lax.axis_index("seq")
    head_count, tokens = step_ref.shape
    width = dy_ref.shape[1]
    rows = x_ref.shape[0]
    chunks, _, lanes = xc.shape
    chunk_heads = lanes // head_width
    groups = recv_x.shape[0]
    group_lanes = width // groups
    group_chunks = chunks // groups

    has_prev = block > 0
    has_next = block < blocks - 1

    barrier = pltpu.get_barrier_semaphore()
    for d in range(1, peers):
        pl.semaphore_signal(
            barrier, inc=1, device_id={"tp": lax.rem(me + d, peers)}, device_id_type=MESH
        )

    @pl.when(has_prev)
    def _():
        pl.semaphore_signal(barrier, inc=1, device_id={"seq": block - 1}, device_id_type=MESH)

    @pl.when(has_next)
    def _():
        pl.semaphore_signal(barrier, inc=1, device_id={"seq": block + 1}, device_id_type=MESH)

    neighbours = jnp.where(has_prev, 1, 0) + jnp.where(has_next, 1, 0)

    own_bc = pltpu.make_async_copy(bc_ref, bcr.at[me], own_sem.at[0])
    load_x = pltpu.make_async_copy(x_ref, x_in, own_sem.at[1])
    own_x = pltpu.make_async_copy(
        x_ref.at[:, pl.ds(pl.multiple_of(me * width, 128), width)], xr.at[me], own_sem.at[2]
    )
    load_step = pltpu.make_async_copy(step_ref, step_in, own_sem.at[3])
    load_dy = pltpu.make_async_copy(dy_ref, dy_in, own_sem.at[4])
    load_rate = pltpu.make_async_copy(rate_ref, rate_sm, own_sem.at[5])
    load_gain = pltpu.make_async_copy(gain_ref, gain_sm, own_sem.at[6])
    own_bc.start()
    load_x.start()
    load_step.start()
    load_dy.start()
    own_x.start()
    load_rate.start()
    load_gain.start()

    def bc_copy(peer, slot):
        return pltpu.make_async_remote_copy(
            src_ref=bcr.at[me], dst_ref=bcr.at[slot],
            send_sem=send_sem.at[0], recv_sem=recv_b.at[0],
            device_id={"tp": peer}, device_id_type=MESH,
        )

    def x_copy(peer, slot, g):
        start = pl.multiple_of(peer * width + g * group_lanes, 128)
        return pltpu.make_async_remote_copy(
            src_ref=x_in.at[:, pl.ds(start, group_lanes)],
            dst_ref=xr.at[slot, :, pl.ds(g * group_lanes, group_lanes)],
            send_sem=send_sem.at[1], recv_sem=recv_x.at[g],
            device_id={"tp": peer}, device_id_type=MESH,
        )

    own_bc.wait()
    pl.semaphore_wait(barrier, peers - 1 + neighbours)
    for d in range(1, peers):
        bc_copy(lax.rem(me + d, peers), me).start()

    early = min(EARLY, groups)

    def lend(source, target, slot, sem, there):
        return pltpu.make_async_remote_copy(
            src_ref=source, dst_ref=target, send_sem=send_sem.at[slot], recv_sem=sem,
            device_id={"seq": there}, device_id_type=MESH,
        )

    def group_of(g):
        return pl.ds(pl.multiple_of(g * group_lanes, 128), group_lanes)

    def lend_x(g):
        part = (slice(None), slice(None), group_of(g))
        return lend(xr.at[part], near_x.at[part], 7, recv_f.at[g * group_chunks], block + 1)

    def lend_dy(g):
        part = (slice(None), group_of(g))
        return lend(dy_in.at[part], next_dy.at[part], 8, recv_g.at[g * group_chunks], block - 1)

    load_step.wait()

    @pl.when(block == 0)
    def _():
        lend(step_in, near_step, 9, recv_n.at[2], block + 1).start()

    load_dy.wait()

    @pl.when(block == blocks - 1)
    def _():
        lend(step_in, next_step, 10, recv_n.at[3], block - 1).start()
        for g in range(early):
            lend_dy(g).start()

    load_x.wait()
    for g in range(groups):
        for d in range(1, peers):
            x_copy(lax.rem(me + d, peers), me, g).start()

    load_rate.wait()
    load_gain.wait()
    stp[...] = jnp.zeros_like(stp)
    stp[0:head_count] = step_in[...]
    rates[...] = jnp.zeros_like(rates)
    gains[...] = jnp.zeros_like(gains)
    for h in range(head_count):
        rates[h : h + 1] = jnp.full((1, tokens), rate_sm[h], F32)
        gains[h : h + 1] = jnp.full((1, tokens), gain_sm[h], F32)
    row = lax.broadcasted_iota(jnp.int32, (tokens, tokens), 0)
    col = lax.broadcasted_iota(jnp.int32, (tokens, tokens), 1)
    upto = row <= col
    cum = exact(-rates[...] * stp[...], jnp.where(upto, 1.0, 0.0).astype(F32))
    cums[...] = cum
    stacked = jnp.concatenate(
        [jnp.exp(cum), jnp.exp(-cum) * stp[...], gains[...], jnp.zeros_like(cum)], axis=0
    )
    table = split(stacked.T)
    pick_row = lax.broadcasted_iota(jnp.int32, (4 * HEAD_PAD, lanes), 0)
    pick_head = lax.broadcasted_iota(jnp.int32, (4 * HEAD_PAD, lanes), 1) // head_width

    def spread(c, q):
        hit = pick_row == (q * HEAD_PAD + c * chunk_heads) + pick_head
        return jnp.where(hit, 1.0, 0.0).astype(BF16)

    for c in range(chunks):
        grown = dot2l(table, spread(c, 0))
        ec[c] = grown
        ed[c] = dot2l(table, spread(c, 1))
        gain_row[c] = dot2l((table[0][0:16], table[1][0:16]), spread(c, 2))[0:8]
        dy = dy_in[:, c * lanes : (c + 1) * lanes]
        dyc[c] = dy
        high, low = split(grown * dy.astype(F32))
        ys_h[c] = high
        ys_l[c] = low

    def forward_copy(c):
        return pltpu.make_async_remote_copy(
            src_ref=code_fo.at[c], dst_ref=code_fi.at[c],
            send_sem=send_sem.at[2], recv_sem=recv_f.at[c],
            device_id={"seq": block + 1}, device_id_type=MESH,
        )

    def backward_copy(c):
        return pltpu.make_async_remote_copy(
            src_ref=code_bo.at[c], dst_ref=code_bi.at[c],
            send_sem=send_sem.at[3], recv_sem=recv_g.at[c],
            device_id={"seq": block - 1}, device_id_type=MESH,
        )

    def landing(ref, sem, slot):
        return pltpu.make_async_remote_copy(
            src_ref=ref, dst_ref=ref, send_sem=send_sem.at[slot], recv_sem=sem,
            device_id={"tp": lax.rem(me + 1, peers)}, device_id_type=MESH,
        )

    def send_forward(c, value):
        code_fo[c] = encode(value)
        forward_copy(c).start()

    def send_backward(c, value):
        code_bo[c] = encode(value)
        backward_copy(c).start()

    def total_decay(c):
        return ec[c, tokens - 1 : tokens, :]

    def borrow(k, steps, weigh):
        landing(steps, recv_n.at[2 + k], 0).wait_recv()
        pads[k] = jnp.zeros_like(pads[k])
        pads[k, 0:head_count] = steps[...]
        cum = exact(-rates[...] * pads[k], jnp.where(upto, 1.0, 0.0).astype(F32))
        filler = jnp.zeros((3 * HEAD_PAD, tokens), F32)
        table = split(jnp.concatenate([weigh(cum, pads[k]), filler], axis=0).T)
        for c in range(chunks):
            weights[k, c] = dot2l(table, spread(c, 0))

    @pl.when(block == 1)
    def _():
        borrow(
            0, near_step,
            lambda cum, steps: jnp.exp(cum[:, tokens - 1 : tokens] - cum) * steps,
        )

    @pl.when(block == blocks - 2)
    def _():
        borrow(1, next_step, lambda cum, steps: jnp.exp(cum))

    landing(bcr.at[pl.ds(0, peers - 1)], recv_b.at[0], 0).wait_recv()

    @pl.when(block == 0)
    def _():
        lend(bcr.at[:, 0], near_b, 6, recv_n.at[0], block + 1).start()

    @pl.when(block == blocks - 1)
    def _():
        lend(bcr.at[:, 1], next_c, 11, recv_n.at[1], block - 1).start()
        for g in range(early, groups):
            lend_dy(g).start()

    proj_b = bcr[:, 0].reshape(tokens, -1)
    proj_c = bcr[:, 1].reshape(tokens, -1)
    bcm[0] = proj_b
    bcm[1] = proj_c
    c_t = proj_c.astype(F32).T.astype(BF16)
    for c in range(chunks):
        pulled[c] = dot2(c_t, (ys_h[c], ys_l[c]))

    b_t = proj_b.astype(F32).T.astype(BF16)
    scores_t = jnp.where(upto, dot(proj_b, proj_c, NT), 0.0)
    sm[0], sm[1] = split(scores_t)
    sm[2], sm[3] = split(scores_t.T)

    @pl.when(jnp.logical_not(has_next))
    def _():
        pull_in[...] = jnp.zeros_like(pull_in)

    dcum_acc[...] = jnp.zeros_like(dcum_acc)
    dir_acc[...] = jnp.zeros_like(dir_acc)

    own_x.wait()
    for g in range(groups):
        group = xr.at[pl.ds(0, peers - 1), :, pl.ds(g * group_lanes, group_lanes)]
        landing(group, recv_x.at[g], 1).wait_recv()

        @pl.when(block == 0)
        def _():
            lend_x(g).start()

        for c in range(g * group_chunks, (g + 1) * group_chunks):
            x = xr[:, :, c * lanes : (c + 1) * lanes].reshape(tokens, lanes)
            xc[c] = x
            pair = split(ed[c] * x.astype(F32))
            xs_h[c] = pair[0]
            xs_l[c] = pair[1]
            fresh[c] = dot2(b_t, pair)

    def finish_inner():
        inner = jnp.zeros((tokens, tokens), F32)
        for c in range(chunks):
            inner += dot3((xs_h[c], xs_l[c]), (ys_h[c], ys_l[c]), NT)
        inner = jnp.where(upto, inner, 0.0)
        bc_acc[0] += dot2l(split(inner), bcm[1])
        bc_acc[1] += dot2l(split(inner.T), bcm[0])

    bc_acc[...] = jnp.zeros_like(bc_acc)

    def sum_copy(q, peer, slot):
        return pltpu.make_async_remote_copy(
            src_ref=bc_acc.at[q, pl.ds(pl.multiple_of(peer * rows, 8), rows)],
            dst_ref=rs.at[q, slot],
            send_sem=send_sem.at[4 + q], recv_sem=recv_r.at[q],
            device_id={"tp": peer}, device_id_type=MESH,
        )

    def send_sums(q):
        for d in range(1, peers):
            sum_copy(q, lax.rem(me + d, peers), me).start()

    def selector(c):
        head = lax.broadcasted_iota(jnp.int32, (HEAD_PAD, lanes), 0)
        of = lax.broadcasted_iota(jnp.int32, (HEAD_PAD, lanes), 1) // head_width
        return jnp.where(head == c * chunk_heads + of, 1.0, 0.0).astype(BF16)

    def rebuilt(k, c, values):
        return dot2(sides[k], split(weights[k, c] * values.astype(F32)))

    def part_of(c):
        return pl.ds(pl.multiple_of(c * lanes, 128), lanes)

    def forward_input(kind, c, opens):
        if kind == "raw":
            if opens:
                group = near_x.at[:, :, pl.ds(0, group_lanes)]
                landing(group, recv_f.at[c], 0).wait_recv()
            entering = rebuilt(0, c, near_x[:, :, part_of(c)].reshape(tokens, lanes))
        else:
            forward_copy(c).wait_recv()
            entering = decode(code_fi[c])
        state_in[c] = entering
        return entering

    def backward_input(kind, c, opens):
        if kind == "raw":
            if opens:
                landing(next_dy.at[:, pl.ds(0, group_lanes)], recv_g.at[c], 0).wait_recv()
            arriving = rebuilt(1, c, next_dy[:, part_of(c)])
        else:
            backward_copy(c).wait_recv()
            arriving = decode(code_bi[c])
        pull_in[c] = arriving
        return arriving

    def forward_link(kind, sends, c, opens):
        if kind == "none":
            state_out[c] = total_decay(c) * fresh[c]
            return
        leaving = total_decay(c) * (forward_input(kind, c, opens) + fresh[c])
        state_out[c] = leaving
        if sends:
            send_forward(c, leaving)

    def backward_link(kind, sends, c, opens):
        if kind == "none":
            return
        arriving = backward_input(kind, c, opens)
        if sends:
            send_backward(c, total_decay(c) * arriving + pulled[c])

    def forward_sum(kind, c):
        if kind != "none":
            bc_acc[1] += dot3((ys_h[c], ys_l[c]), split(state_in[c]), NT)

    def backward_sum(kind, c):
        if kind != "none":
            leaving = split(total_decay(c) * pull_in[c])
            bc_acc[0] += dot3((xs_h[c], xs_l[c]), leaving, NT)

    def forward_work(kind, c):
        left, right = (sm[2], sm[2], sm[3]), (xs_h[c], xs_l[c], xs_h[c])
        if kind != "none":
            left, right = (*left, bcm[1], bcm[1]), (*right, *split(state_in[c]))
        z = joined(left, right)
        v = split(ec[c] * dyc[c].astype(F32) * z)
        dcum_acc[...] += dot2(selector(c), v, NT)

    def backward_work(kind, c):
        left, right = (sm[0], sm[0], sm[1]), (ys_h[c], ys_l[c], ys_h[c])
        if kind != "none":
            leaving = split(total_decay(c) * pull_in[c])
            left, right = (*left, bcm[0], bcm[0]), (*right, *leaving)
        a2 = joined(left, right)
        x = xc[c].astype(F32)
        growth = ed[c]
        gx = growth * a2 + gain_row[c, 0:1, :] * dyc[c].astype(F32)
        gx_ref[:, part_of(c)] = gx.astype(BF16)
        direct = x * a2
        pick = selector(c)
        dir_acc[...] += dot2(pick, split(direct), NT)
        dcum_acc[...] -= dot2(pick, split(growth * direct), NT)

    def grouped(part, *fixed):
        def run(g):
            for i in range(group_chunks):
                part(*fixed, g * group_chunks + i)
        return run

    def grouped_link(part, kind, sends):
        def run(g):
            for i in range(group_chunks):
                part(kind, sends, g * group_chunks + i, i == 0)
        return run

    def loop(low, high, *parts):
        def body(k, carry):
            for part, shift in parts:
                part(k + shift)
            return carry

        if high > low:
            lax.fori_loop(low, high, body, 0)

    def edge_role(links, sums, work, other_work, early, late):
        finish_inner()
        send_sums(early)
        loop(0, groups, (other_work, 0))
        loop(0, groups - 1, (links, 0), (sums, 0), (work, 0))
        links(groups - 1)
        sums(groups - 1)
        send_sums(late)
        work(groups - 1)

    def inner_role(lead, follow, lag):
        (link1, sum1, work1), (link2, sum2, work2) = lead, follow
        ahead = min(lag, groups)
        rest = groups - ahead
        both = min(ahead, rest)
        loop(0, ahead, (link1, 0), (sum1, 0), (work1, 0))
        loop(ahead, groups, (link1, 0), (link2, -ahead))
        loop(
            rest, rest + both, (link2, 0), (sum1, ahead - rest), (work1, ahead - rest),
            (sum2, -rest), (work2, -rest),
        )
        loop(rest + both, groups, (link2, 0), (sum2, -rest), (work2, -rest))
        loop(ahead + both, groups, (sum1, 0))
        loop(ahead, groups, (sum2, 0))
        finish_inner()
        send_sums(0)
        send_sums(1)
        loop(ahead + both, groups, (work1, 0))
        loop(ahead, groups, (work2, 0))

    def between(s, carry):
        cf = s - SKEW * (block - 1)
        cb = s - SKEW * (blocks - 2 - block)

        @pl.when(jnp.logical_and(cf >= 0, cf < chunks))
        def _():
            forward_link("code", True, cf, True)
            forward_sum("code", cf)
            forward_work("code", cf)

        @pl.when(jnp.logical_and(cb >= 0, cb < chunks))
        def _():
            backward_link("code", True, cb, True)
            backward_sum("code", cb)
            backward_work("code", cb)

        return carry

    special = sorted({0, 1, blocks - 2, blocks - 1})
    for b in special:
        @pl.when(block == b)
        def _():
            forward = "none" if b == 0 else "raw" if b == 1 else "code"
            backward = "none" if b == blocks - 1 else "raw" if b == blocks - 2 else "code"
            if forward == "raw":
                landing(near_b, recv_n.at[0], 0).wait_recv()
                sides[0] = near_b[...].reshape(tokens, -1).astype(F32).T.astype(BF16)
            if backward == "raw":
                landing(next_c, recv_n.at[1], 0).wait_recv()
                sides[1] = next_c[...].reshape(tokens, -1).astype(F32).T.astype(BF16)
            sends = forward != "none" and backward != "none"
            ahead = (
                grouped_link(forward_link, forward, sends),
                grouped(forward_sum, forward), grouped(forward_work, forward),
            )
            behind = (
                grouped_link(backward_link, backward, sends),
                grouped(backward_sum, backward), grouped(backward_work, backward),
            )
            if forward == "none":
                loop(0, groups, (ahead[0], 0))
                edge_role(*behind, ahead[2], 1, 0)
            elif backward == "none":
                edge_role(*ahead, behind[2], 0, 1)
            else:
                lag = LAG * ((blocks - 2 - b) - (b - 1))
                if lag < 0:
                    ahead, behind = behind, ahead
                inner_role(ahead, behind, abs(lag))

    if blocks > 4:
        @pl.when(jnp.logical_and(block > 1, block < blocks - 2))
        def _():
            lax.fori_loop(0, chunks + SKEW * (blocks - 3), between, 0)
            finish_inner()
            send_sums(1)
            send_sums(0)

    edge = jnp.zeros((HEAD_PAD, 8), F32)
    for c in range(chunks):
        both = (pull_in[c] * state_out[c]).reshape(-1, 8, lanes).sum(axis=0)
        edge = edge + dot2(selector(c), split(both), NT)
    edge = jnp.sum(edge, axis=1, keepdims=True)
    after = exact(dcum_acc[...], jnp.where(row >= col, 1.0, 0.0).astype(F32)) + edge
    gstep = jnp.exp(-cums[...]) * dir_acc[...] - rates[...] * after
    gstep_ref[...] = gstep[0:head_count]

    for q in range(2):
        landing(rs.at[q, pl.ds(0, peers - 1)], recv_r.at[q], 4 + q).wait_recv()
        total = bc_acc[q, pl.ds(pl.multiple_of(me * rows, 8), rows)]
        for d in range(1, peers):
            total = total + rs[q, lax.rem(me + d, peers)]
        gbc_ref[q] = total

    landing(bcr.at[pl.ds(0, peers - 1)], recv_b.at[0], 0).wait_send()
    landing(xr.at[pl.ds(0, peers - 1)], recv_x.at[0], 1).wait_send()
    for q in range(2):
        landing(rs.at[q, pl.ds(0, peers - 1)], recv_r.at[q], 4 + q).wait_send()

    inner_block = jnp.logical_and(has_prev, has_next)

    @pl.when(inner_block)
    def _():
        landing(code_fo, recv_f.at[0], 2).wait_send()
        landing(code_bo, recv_g.at[0], 3).wait_send()

    @pl.when(block == 0)
    def _():
        landing(near_b, recv_n.at[0], 6).wait_send()
        landing(near_step, recv_n.at[2], 9).wait_send()
        landing(near_x, recv_f.at[0], 7).wait_send()

    @pl.when(block == blocks - 1)
    def _():
        landing(next_c, recv_n.at[1], 11).wait_send()
        landing(next_step, recv_n.at[3], 10).wait_send()
        landing(dy_in, recv_g.at[0], 8).wait_send()


def store(gx_ref, gbc_ref, gstep_ref, gx_out, gbc_out, gstep_out, sems):
    copies = [
        pltpu.make_async_copy(source, target, sems.at[k])
        for k, (source, target) in enumerate(
            ((gx_ref, gx_out), (gbc_ref, gbc_out), (gstep_ref, gstep_out))
        )
    ]
    for copy in copies:
        copy.start()
    for copy in copies:
        copy.wait()


def shards(x_ckpt, bc_ckpt, step_sizes, decay_rate, skip_gain, grad_out):
    peers, blocks = lax.axis_size("tp"), lax.axis_size("seq")
    rows = x_ckpt.shape[0]
    head_count, tokens = step_sizes.shape
    width = grad_out.shape[1]
    state = bc_ckpt.shape[2]
    lanes = 128
    chunks = width // lanes
    head_width = width // head_count
    groups = chunks // 2 if chunks % 2 == 0 else chunks
    wide = lambda dtype, size: pltpu.VMEM((chunks, size, lanes), dtype)
    dma = lambda n: pltpu.SemaphoreType.DMA((n,))
    vmem = pl.BlockSpec(memory_space=pltpu.VMEM)
    hbm = pl.BlockSpec(memory_space=pl.ANY)
    heads = pltpu.VMEM((HEAD_PAD, tokens), F32)
    outs = (
        ((tokens, width), BF16),
        ((2, rows, state), F32),
        ((head_count, tokens), F32),
    )
    grads = pl.pallas_call(
        partial(kernel, peers, blocks, head_width),
        out_shape=tuple(pltpu.VMEM(shape, dtype) for shape, dtype in outs),
        in_specs=[hbm] * 6,
        out_specs=(vmem, vmem, vmem),
        scratch_shapes=[
            pltpu.VMEM(x_ckpt.shape, BF16),
            pltpu.VMEM((tokens, width), BF16),
            pltpu.VMEM((head_count, tokens), F32),
            pltpu.VMEM((peers, rows, width), BF16),
            pltpu.VMEM((peers, 2, rows, state), BF16),
            pltpu.VMEM((2, peers, rows, state), F32),
            *[wide(F32, state)] * 5,
            *[wide(BF16, state + TOP_ROWS)] * 4,
            pltpu.VMEM((peers, rows, width), BF16),
            pltpu.VMEM((peers, rows, state), BF16),
            pltpu.VMEM((head_count, tokens), F32),
            pltpu.VMEM((tokens, width), BF16),
            pltpu.VMEM((peers, rows, state), BF16),
            pltpu.VMEM((head_count, tokens), F32),
            pltpu.VMEM((2, HEAD_PAD, tokens), F32),
            pltpu.VMEM((2, chunks, tokens, lanes), F32),
            pltpu.VMEM((2, state, tokens), BF16),
            *[wide(BF16, tokens)] * 6,
            *[wide(F32, tokens)] * 2,
            wide(F32, 8),
            heads, heads, heads, heads,
            pltpu.VMEM((2, tokens, state), F32),
            heads, heads,
            pltpu.VMEM((4, tokens, tokens), BF16),
            pltpu.VMEM((2, tokens, state), BF16),
            pltpu.SMEM((head_count,), F32), pltpu.SMEM((head_count,), F32),
            dma(7), dma(12), dma(groups), dma(1), dma(chunks), dma(chunks), dma(2), dma(4),
        ],
        compiler_params=pltpu.CompilerParams(collective_id=0, has_side_effects=True),
    )(x_ckpt, bc_ckpt, step_sizes, decay_rate, skip_gain, grad_out)
    return pl.pallas_call(
        store,
        out_shape=tuple(jax.ShapeDtypeStruct(shape, dtype) for shape, dtype in outs),
        in_specs=[vmem] * 3,
        out_specs=(hbm,) * 3,
        scratch_shapes=[dma(3)],
    )(*[pltpu.with_memory_space_constraint(grad, pltpu.VMEM) for grad in grads])


def solution(mesh):
    return jax.shard_map(
        shards,
        mesh=mesh,
        in_specs=(
            P(("dp", "seq", "tp"), None),
            P(None, ("dp", "seq", "tp"), None),
            P("tp", ("dp", "seq")),
            P("tp"),
            P("tp"),
            P(("dp", "seq"), "tp"),
        ),
        out_specs=(
            P(("dp", "seq"), "tp"),
            P(None, ("dp", "seq", "tp"), None),
            P("tp", ("dp", "seq")),
        ),
        check_vma=False,
    )
```

```python
import math
from functools import partial

import jax
import jax.numpy as jnp
from jax import lax
from jax.experimental import pallas as pl
from jax.experimental.pallas import tpu as pltpu
from jax.sharding import PartitionSpec as P

MESH = pl.DeviceIdType.MESH
F32 = jnp.float32
BF16 = jnp.bfloat16
HEAD_PAD = 32
SKEW = 4
FOLLOW_FORWARD = 3
FOLLOW_BACK = 4
WORK_EVERY = 30
DIRECT = 2
SPAN = 125.0
TOP_ROWS = 8

NN = (((1,), (0,)), ((), ()))
NT = (((1,), (1,)), ((), ()))


def dot(a, b, dims=NN):
    return lax.dot_general(a, b, dims, preferred_element_type=F32)


def exact(a, b):
    return lax.dot_general(
        a, b, NN, precision=lax.Precision.HIGHEST, preferred_element_type=F32
    )


def split(v):
    high = v.astype(BF16)
    return high, (v - high.astype(F32)).astype(BF16)


def joined(a, b, dims=NN):
    return dot(jnp.concatenate(a, axis=1), jnp.concatenate(b, axis=dims[0][1][0]), dims)


def dot2(a, b, dims=NN):
    return joined((a, a), b, dims)


def dot2l(a, b, dims=NN):
    return joined(a, (b, b), dims)


def dot3(a, b, dims=NN):
    return joined((a[0], a[0], a[1]), (b[0], b[1], b[0]), dims)


def encode(v):
    top = jnp.max(jnp.abs(v), axis=0, keepdims=True)
    top = jnp.maximum(top, 1e-30).astype(BF16)
    code = jnp.exp2(v * (SPAN / top.astype(F32))).astype(BF16)
    return jnp.concatenate([code, jnp.broadcast_to(top, (TOP_ROWS, v.shape[1]))], axis=0)


def decode(message):
    size = message.shape[0] - TOP_ROWS
    top = message[size : size + 1].astype(F32)
    return jnp.log(message[0:size].astype(F32)) * (top * (1.0 / (SPAN * math.log(2.0))))


def kernel(
    peers, blocks, head_width,
    x_ref, bc_ref, step_ref, rate_ref, gain_ref, dy_ref,
    gx_ref, gbc_ref, gstep_ref,
    x_in, dy_in, step_in, xr, bcr, rs,
    state_in, state_out, pull_in, fresh, pulled,
    code_fo, code_fi, code_bo, code_bi,
    near_x, near_b, near_step, next_dy, next_c, next_step, pads, weights, sides,
    xs_h, xs_l, ys_h, ys_l, xc, dyc, ec, ed, gain_row,
    stp, rates, gains, cums, bc_acc, dcum_acc, dir_acc, sm, bcm, turned,
    rate_sm, gain_sm, own_sem, send_sem, recv_x, recv_b, recv_f, recv_g, recv_r, recv_n,
):
    me = lax.axis_index("tp")
    block = lax.axis_index("seq")
    head_count, tokens = step_ref.shape
    width = dy_ref.shape[1]
    rows = x_ref.shape[0]
    chunks, _, lanes = xc.shape
    chunk_heads = lanes // head_width
    groups = recv_x.shape[0]
    group_lanes = width // groups
    group_chunks = chunks // groups

    has_prev = block > 0
    has_next = block < blocks - 1

    mirror = peers - 1 - me
    if peers % 2 == 0:
        partners = [mirror]
        for i in range(2, peers, 2):
            partners += [lax.rem(me + i, peers), lax.rem(mirror + i, peers)]
    else:
        partners = [lax.rem(me + d, peers) for d in range(1, peers)]

    barrier = pltpu.get_barrier_semaphore()
    for peer in partners:
        pl.semaphore_signal(barrier, inc=1, device_id={"tp": peer}, device_id_type=MESH)

    def greet(there, exists, wide):
        @pl.when(jnp.logical_and(exists, wide))
        def _():
            for peer in range(peers):
                pl.semaphore_signal(
                    barrier, inc=1, device_id={"seq": there, "tp": peer}, device_id_type=MESH
                )

        @pl.when(jnp.logical_and(exists, jnp.logical_not(wide)))
        def _():
            pl.semaphore_signal(barrier, inc=1, device_id={"seq": there}, device_id_type=MESH)

        return jnp.where(exists, jnp.where(wide, peers, 1), 0)

    greeted = greet(block - 1, has_prev, jnp.logical_or(block == 1, block == blocks - 1))
    greeted += greet(block + 1, has_next, jnp.logical_or(block == 0, block == blocks - 2))

    own_bc = pltpu.make_async_copy(bc_ref, bcr.at[me], own_sem.at[0])
    load_x = pltpu.make_async_copy(x_ref, x_in, own_sem.at[1])
    own_x = pltpu.make_async_copy(
        x_ref.at[:, pl.ds(pl.multiple_of(me * width, 128), width)], xr.at[me], own_sem.at[2]
    )
    load_step = pltpu.make_async_copy(step_ref, step_in, own_sem.at[3])
    load_dy = pltpu.make_async_copy(dy_ref, dy_in, own_sem.at[4])
    load_rate = pltpu.make_async_copy(rate_ref, rate_sm, own_sem.at[5])
    load_gain = pltpu.make_async_copy(gain_ref, gain_sm, own_sem.at[6])
    own_bc.start()
    load_x.start()
    load_step.start()
    load_dy.start()
    own_x.start()
    load_rate.start()
    load_gain.start()

    def bc_copy(peer, slot):
        return pltpu.make_async_remote_copy(
            src_ref=bcr.at[me], dst_ref=bcr.at[slot],
            send_sem=send_sem.at[0], recv_sem=recv_b.at[0],
            device_id={"tp": peer}, device_id_type=MESH,
        )

    def x_copy(peer, slot, g):
        start = pl.multiple_of(peer * width + g * group_lanes, 128)
        return pltpu.make_async_remote_copy(
            src_ref=x_in.at[:, pl.ds(start, group_lanes)],
            dst_ref=xr.at[slot, :, pl.ds(g * group_lanes, group_lanes)],
            send_sem=send_sem.at[1], recv_sem=recv_x.at[g],
            device_id={"tp": peer}, device_id_type=MESH,
        )

    own_bc.wait()
    load_step.wait()
    pl.semaphore_wait(barrier, peers - 1 + greeted)

    def lend(source, target, slot, sem, there):
        return pltpu.make_async_remote_copy(
            src_ref=source, dst_ref=target, send_sem=send_sem.at[slot], recv_sem=sem,
            device_id={"seq": there}, device_id_type=MESH,
        )

    def lend_row(q, target, slot, sem, peer, there):
        return pltpu.make_async_remote_copy(
            src_ref=bcr.at[me, q], dst_ref=target.at[me],
            send_sem=send_sem.at[slot], recv_sem=sem,
            device_id={"seq": there, "tp": peer}, device_id_type=MESH,
        )

    @pl.when(block == 0)
    def _():
        lend(step_in, near_step, 9, recv_n.at[2], block + 1).start()
        for peer in (*partners, me):
            lend_row(0, near_b, 6, recv_n.at[0], peer, block + 1).start()

    @pl.when(block == blocks - 1)
    def _():
        lend(step_in, next_step, 10, recv_n.at[3], block - 1).start()
        for peer in (*partners, me):
            lend_row(1, next_c, 11, recv_n.at[1], peer, block - 1).start()

    for peer in partners:
        bc_copy(peer, me).start()

    direct = min(DIRECT, groups)

    def lend_x(c, slot):
        part = (slot, slice(None), pl.ds(c * lanes, lanes))
        return lend(xr.at[part], near_x.at[part], 7, recv_f.at[c], block + 1)

    def lend_own_x():
        part = (me, slice(None), pl.ds(direct * group_lanes, width - direct * group_lanes))
        return lend(xr.at[part], near_x.at[part], 7, recv_n.at[4], block + 1)

    def lend_direct(c, peer):
        start = pl.multiple_of(peer * width + c * lanes, 128)
        return pltpu.make_async_remote_copy(
            src_ref=x_in.at[:, pl.ds(start, lanes)],
            dst_ref=near_x.at[me, :, pl.ds(c * lanes, lanes)],
            send_sem=send_sem.at[7], recv_sem=recv_f.at[c],
            device_id={"seq": block + 1, "tp": peer}, device_id_type=MESH,
        )

    def lend_dy(c):
        part = (slice(None), pl.ds(c * lanes, lanes))
        return lend(dy_in.at[part], next_dy.at[part], 8, recv_g.at[c], block - 1)

    load_dy.wait()

    @pl.when(block == blocks - 1)
    def _():
        for c in range(chunks):
            lend_dy(c).start()

    load_x.wait()
    own_x.wait()
    for g in range(groups):
        if g < direct:
            @pl.when(block == 0)
            def _():
                for c in range(g * group_chunks, (g + 1) * group_chunks):
                    for peer in (*partners, me):
                        lend_direct(c, peer).start()

        if g == direct:
            @pl.when(block == 0)
            def _():
                lend_own_x().start()

        for peer in partners:
            x_copy(peer, me, g).start()

    load_rate.wait()
    load_gain.wait()
    stp[...] = jnp.zeros_like(stp)
    stp[0:head_count] = step_in[...]
    rates[...] = jnp.zeros_like(rates)
    gains[...] = jnp.zeros_like(gains)
    for h in range(head_count):
        rates[h : h + 1] = jnp.full((1, tokens), rate_sm[h], F32)
        gains[h : h + 1] = jnp.full((1, tokens), gain_sm[h], F32)
    row = lax.broadcasted_iota(jnp.int32, (tokens, tokens), 0)
    col = lax.broadcasted_iota(jnp.int32, (tokens, tokens), 1)
    upto = row <= col
    cum = exact(-rates[...] * stp[...], jnp.where(upto, 1.0, 0.0).astype(F32))
    cums[...] = cum
    stacked = jnp.concatenate(
        [jnp.exp(cum), jnp.exp(-cum) * stp[...], gains[...], jnp.zeros_like(cum)], axis=0
    )
    table = split(stacked.T)
    pick_row = lax.broadcasted_iota(jnp.int32, (4 * HEAD_PAD, lanes), 0)
    pick_head = lax.broadcasted_iota(jnp.int32, (4 * HEAD_PAD, lanes), 1) // head_width

    def spread(c, q):
        hit = pick_row == (q * HEAD_PAD + c * chunk_heads) + pick_head
        return jnp.where(hit, 1.0, 0.0).astype(BF16)

    for c in range(chunks):
        grown = dot2l(table, spread(c, 0))
        ec[c] = grown
        ed[c] = dot2l(table, spread(c, 1))
        gain_row[c] = dot2l((table[0][0:16], table[1][0:16]), spread(c, 2))[0:8]
        dy = dy_in[:, c * lanes : (c + 1) * lanes]
        dyc[c] = dy
        high, low = split(grown * dy.astype(F32))
        ys_h[c] = high
        ys_l[c] = low

    def forward_copy(c):
        return pltpu.make_async_remote_copy(
            src_ref=code_fo.at[c], dst_ref=code_fi.at[c],
            send_sem=send_sem.at[2], recv_sem=recv_f.at[c],
            device_id={"seq": block + 1}, device_id_type=MESH,
        )

    def backward_copy(c):
        return pltpu.make_async_remote_copy(
            src_ref=code_bo.at[c], dst_ref=code_bi.at[c],
            send_sem=send_sem.at[3], recv_sem=recv_g.at[c],
            device_id={"seq": block - 1}, device_id_type=MESH,
        )

    def landing(ref, sem, slot):
        return pltpu.make_async_remote_copy(
            src_ref=ref, dst_ref=ref, send_sem=send_sem.at[slot], recv_sem=sem,
            device_id={"tp": lax.rem(me + 1, peers)}, device_id_type=MESH,
        )

    def send_forward(c, value):
        code_fo[c] = encode(value)
        forward_copy(c).start()

    def send_backward(c, value):
        code_bo[c] = encode(value)
        backward_copy(c).start()

    def total_decay(c):
        return ec[c, tokens - 1 : tokens, :]

    def borrow(k, steps, weigh):
        landing(steps, recv_n.at[2 + k], 0).wait_recv()
        pads[k] = jnp.zeros_like(pads[k])
        pads[k, 0:head_count] = steps[...]
        cum = exact(-rates[...] * pads[k], jnp.where(upto, 1.0, 0.0).astype(F32))
        filler = jnp.zeros((3 * HEAD_PAD, tokens), F32)
        table = split(jnp.concatenate([weigh(cum, pads[k]), filler], axis=0).T)
        for c in range(chunks):
            weights[k, c] = dot2l(table, spread(c, 0))

    def borrow_side(k, side):
        landing(side, recv_n.at[k], 0).wait_recv()
        sides[k] = side[...].reshape(tokens, -1).astype(F32).T.astype(BF16)

    def gather_bc():
        landing(bcr.at[pl.ds(0, peers - 1)], recv_b.at[0], 0).wait_recv()
        proj_b = bcr[:, 0].reshape(tokens, -1)
        proj_c = bcr[:, 1].reshape(tokens, -1)
        bcm[0] = proj_b
        bcm[1] = proj_c
        turned[0] = proj_b.astype(F32).T.astype(BF16)
        turned[1] = proj_c.astype(F32).T.astype(BF16)
        scores_t = jnp.where(upto, dot(proj_b, proj_c, NT), 0.0)
        sm[0], sm[1] = split(scores_t)
        sm[2], sm[3] = split(scores_t.T)

    def pull_all():
        for c in range(chunks):
            pulled[c] = dot2(turned[1], (ys_h[c], ys_l[c]))

    def take_x(g):
        group = xr.at[pl.ds(0, peers - 1), :, pl.ds(g * group_lanes, group_lanes)]
        landing(group, recv_x.at[g], 1).wait_recv()
        if g >= direct:
            @pl.when(block == 0)
            def _():
                for c in range(g * group_chunks, (g + 1) * group_chunks):
                    for peer in partners:
                        lend_x(c, peer).start()

        for c in range(g * group_chunks, (g + 1) * group_chunks):
            x = xr[:, :, c * lanes : (c + 1) * lanes].reshape(tokens, lanes)
            xc[c] = x
            pair = split(ed[c] * x.astype(F32))
            xs_h[c] = pair[0]
            xs_l[c] = pair[1]
            fresh[c] = dot2(turned[0], pair)

    @pl.when(jnp.logical_not(has_next))
    def _():
        pull_in[...] = jnp.zeros_like(pull_in)

    dcum_acc[...] = jnp.zeros_like(dcum_acc)
    dir_acc[...] = jnp.zeros_like(dir_acc)

    def finish_inner():
        inner = jnp.zeros((tokens, tokens), F32)
        for c in range(chunks):
            inner += dot3((xs_h[c], xs_l[c]), (ys_h[c], ys_l[c]), NT)
        inner = jnp.where(upto, inner, 0.0)
        bc_acc[0] += dot2l(split(inner), bcm[1])
        bc_acc[1] += dot2l(split(inner.T), bcm[0])

    bc_acc[...] = jnp.zeros_like(bc_acc)

    def sum_copy(q, peer, slot):
        return pltpu.make_async_remote_copy(
            src_ref=bc_acc.at[q, pl.ds(pl.multiple_of(peer * rows, 8), rows)],
            dst_ref=rs.at[q, slot],
            send_sem=send_sem.at[4 + q], recv_sem=recv_r.at[q],
            device_id={"tp": peer}, device_id_type=MESH,
        )

    def send_sums(q):
        for peer in partners:
            sum_copy(q, peer, me).start()

    def selector(c):
        head = lax.broadcasted_iota(jnp.int32, (HEAD_PAD, lanes), 0)
        of = lax.broadcasted_iota(jnp.int32, (HEAD_PAD, lanes), 1) // head_width
        return jnp.where(head == c * chunk_heads + of, 1.0, 0.0).astype(BF16)

    def rebuilt(k, c, values):
        return dot2(sides[k], split(weights[k, c] * values.astype(F32)))

    def part_of(c):
        if isinstance(c, int):
            return pl.ds(c * lanes, lanes)
        return pl.ds(pl.multiple_of(c * lanes, 128), lanes)

    def forward_input(kind, c):
        if kind == "raw":
            if c == direct * group_chunks:
                rest = width - c * lanes
                landing(near_x.at[0, :, pl.ds(0, rest)], recv_n.at[4], 0).wait_recv()
            count = peers if c < direct * group_chunks else peers - 1
            part = near_x.at[pl.ds(0, count), :, pl.ds(0, lanes)]
            landing(part, recv_f.at[c], 0).wait_recv()
            entering = rebuilt(0, c, near_x[:, :, part_of(c)].reshape(tokens, lanes))
        else:
            forward_copy(c).wait_recv()
            entering = decode(code_fi[c])
        state_in[c] = entering
        return entering

    def backward_input(kind, c):
        if kind == "raw":
            landing(next_dy.at[:, pl.ds(0, lanes)], recv_g.at[c], 0).wait_recv()
            arriving = rebuilt(1, c, next_dy[:, part_of(c)])
        else:
            backward_copy(c).wait_recv()
            arriving = decode(code_bi[c])
        pull_in[c] = arriving
        return arriving

    def forward_link(kind, sends, c):
        if kind == "none":
            state_out[c] = total_decay(c) * fresh[c]
            return

        leaving = total_decay(c) * (forward_input(kind, c) + fresh[c])
        state_out[c] = leaving
        if sends:
            send_forward(c, leaving)

    def backward_link(kind, sends, c):
        if kind == "none":
            return
        arriving = backward_input(kind, c)
        if sends:
            send_backward(c, total_decay(c) * arriving + pulled[c])

    def forward_sum(kind, c):
        if kind != "none":
            bc_acc[1] += dot3((ys_h[c], ys_l[c]), split(state_in[c]), NT)

    def backward_sum(kind, c):
        if kind != "none":
            leaving = split(total_decay(c) * pull_in[c])
            bc_acc[0] += dot3((xs_h[c], xs_l[c]), leaving, NT)

    def forward_work(kind, c):
        left, right = (sm[2], sm[2], sm[3]), (xs_h[c], xs_l[c], xs_h[c])
        if kind != "none":
            left, right = (*left, bcm[1], bcm[1]), (*right, *split(state_in[c]))
        z = joined(left, right)
        dcum_acc[...] += dot2(selector(c), split(dyc[c].astype(F32) * z), NT)

    def backward_work(kind, c):
        left, right = (sm[0], sm[0], sm[1]), (ys_h[c], ys_l[c], ys_h[c])
        if kind != "none":
            leaving = split(total_decay(c) * pull_in[c])
            left, right = (*left, bcm[0], bcm[0]), (*right, *leaving)
        a2 = joined(left, right)
        x = xc[c].astype(F32)
        gx = ed[c] * a2 + gain_row[c, 0:1, :] * dyc[c].astype(F32)
        gx_ref[:, part_of(c)] = gx.astype(BF16)
        dir_acc[...] += dot2(selector(c), split(x * a2), NT)

    def grouped(part, *fixed):
        def run(g):
            for i in range(group_chunks):
                part(*fixed, g * group_chunks + i)
        return run

    def loop(low, high, *parts):
        def body(k, carry):
            for part, shift in parts:
                part(k + shift)
            return carry

        if high > low:
            lax.fori_loop(low, high, body, 0)

    def edge_role(link, add, work, other_work, early, late, flat):
        def take(g):
            for i in range(group_chunks):
                link(g * group_chunks + i)
                add(g * group_chunks + i)

        finish_inner()
        send_sums(early)
        loop(0, groups, (other_work, 0))
        if flat:
            for g in range(groups - 1):
                take(g)
                work(g)
        else:
            loop(0, groups - 1, (take, 0), (work, 0))
        take(groups - 1)
        send_sums(late)
        work(groups - 1)

    def inner_role(lead, follow, behind, done):
        (link1, add1, work1), (link2, add2, work2) = lead, follow
        links, adds, works = (link1, link2), (add1, add2), (work1, work2)
        steps = [(0, c) for c in range(chunks)]
        for c in reversed(range(chunks)):
            steps.insert(min(chunks, behind + 3 * c // 2 + 1), (1, c))
        ready = [(0, c) for c in range(group_chunks - 1, done, group_chunks)]
        steps = [step for step in steps if step not in [(0, c) for c in range(done)]]

        def add_group(side, g):
            for c in range(g * group_chunks, (g + 1) * group_chunks):
                adds[side](c)

        for at, (side, c) in enumerate(steps):
            links[side](c)
            if c % group_chunks == group_chunks - 1:
                ready.append((side, c))
            leading = any(other == 0 for other, _ in steps[at + 1 :])
            if ready and (not leading or at % WORK_EVERY == WORK_EVERY - 1):
                other, last = ready.pop(0)
                add_group(other, last // group_chunks)
                works[other](last // group_chunks)
        for side, last in ready:
            add_group(side, last // group_chunks)
        finish_inner()
        send_sums(0)
        send_sums(1)
        for side, last in ready:
            works[side](last // group_chunks)

    def between(s, carry):
        cf = s - SKEW * (block - 1)
        cb = s - SKEW * (blocks - 2 - block)

        @pl.when(jnp.logical_and(cf >= 0, cf < chunks))
        def _():
            forward_link("code", True, cf)
            forward_sum("code", cf)
            forward_work("code", cf)

        @pl.when(jnp.logical_and(cb >= 0, cb < chunks))
        def _():
            backward_link("code", True, cb)
            backward_sum("code", cb)
            backward_work("code", cb)

        return carry

    special = sorted({0, 1, blocks - 2, blocks - 1})
    for b in special:
        @pl.when(block == b)
        def _():
            forward = "none" if b == 0 else "raw" if b == 1 else "code"
            backward = "none" if b == blocks - 1 else "raw" if b == blocks - 2 else "code"
            sends = forward != "none" and backward != "none"
            ahead = (
                partial(forward_link, forward, sends),
                partial(forward_sum, forward), grouped(forward_work, forward),
            )
            behind = (
                partial(backward_link, backward, sends),
                partial(backward_sum, backward), grouped(backward_work, backward),
            )
            lag = (blocks - 2 - b) - (b - 1)
            if forward == "raw":
                borrow(
                    0, near_step,
                    lambda cum, steps: jnp.exp(cum[:, tokens - 1 : tokens] - cum) * steps,
                )
            if backward == "raw":
                borrow(1, next_step, lambda cum, steps: jnp.exp(cum))
            gather_bc()
            if sends:
                pull_all()
            if forward == "raw":
                borrow_side(0, near_b)
            if backward == "raw":
                borrow_side(1, next_c)
            done = 0
            if sends and lag < 0:
                done = group_chunks
                for c in range(done):
                    behind[0](c)
            for g in range(groups):
                take_x(g)
                if sends and lag > 0 and g < direct:
                    done = (g + 1) * group_chunks
                    for c in range(g * group_chunks, done):
                        ahead[0](c)
            if forward == "none":
                loop(0, groups, (grouped(ahead[0]), 0))
                edge_role(*behind, ahead[2], 1, 0, backward == "raw")
            elif backward == "none":
                edge_role(*ahead, behind[2], 0, 1, forward == "raw")
            elif lag < 0:
                inner_role(behind, ahead, FOLLOW_FORWARD - 3 * (lag + 1), done)
            else:
                inner_role(ahead, behind, FOLLOW_BACK + 3 * max(lag - 1, 0), done)

    if blocks > 4:
        @pl.when(jnp.logical_and(block > 1, block < blocks - 2))
        def _():
            gather_bc()
            pull_all()
            for g in range(groups):
                take_x(g)
            lax.fori_loop(0, chunks + SKEW * (blocks - 3), between, 0)
            finish_inner()
            send_sums(1)
            send_sums(0)

    edge = jnp.zeros((HEAD_PAD, 8), F32)
    for c in range(chunks):
        both = (pull_in[c] * state_out[c]).reshape(-1, 8, lanes).sum(axis=0)
        edge = edge + dot2(selector(c), split(both), NT)
    edge = jnp.sum(edge, axis=1, keepdims=True)
    growth = jnp.exp(-cums[...])
    dcum = jnp.exp(cums[...]) * dcum_acc[...] - growth * stp[...] * dir_acc[...]
    after = exact(dcum, jnp.where(row >= col, 1.0, 0.0).astype(F32)) + edge
    gstep = growth * dir_acc[...] - rates[...] * after
    gstep_ref[...] = gstep[0:head_count]

    for q in range(2):
        landing(rs.at[q, pl.ds(0, peers - 1)], recv_r.at[q], 4 + q).wait_recv()
        total = bc_acc[q, pl.ds(pl.multiple_of(me * rows, 8), rows)]
        for peer in partners:
            total = total + rs[q, peer]
        gbc_ref[q] = total

    landing(bcr.at[pl.ds(0, peers - 1)], recv_b.at[0], 0).wait_send()
    landing(xr.at[pl.ds(0, peers - 1)], recv_x.at[0], 1).wait_send()
    for q in range(2):
        landing(rs.at[q, pl.ds(0, peers - 1)], recv_r.at[q], 4 + q).wait_send()

    inner_block = jnp.logical_and(has_prev, has_next)

    @pl.when(inner_block)
    def _():
        landing(code_fo, recv_f.at[0], 2).wait_send()
        landing(code_bo, recv_g.at[0], 3).wait_send()

    @pl.when(block == 0)
    def _():
        landing(near_b, recv_n.at[0], 6).wait_send()
        landing(near_step, recv_n.at[2], 9).wait_send()
        landing(near_x, recv_f.at[0], 7).wait_send()

    @pl.when(block == blocks - 1)
    def _():
        landing(next_c, recv_n.at[1], 11).wait_send()
        landing(next_step, recv_n.at[3], 10).wait_send()
        landing(dy_in, recv_g.at[0], 8).wait_send()


def store(gx_ref, gbc_ref, gstep_ref, gx_out, gbc_out, gstep_out, sems):
    copies = [
        pltpu.make_async_copy(source, target, sems.at[k])
        for k, (source, target) in enumerate(
            ((gx_ref, gx_out), (gbc_ref, gbc_out), (gstep_ref, gstep_out))
        )
    ]
    for copy in copies:
        copy.start()
    for copy in copies:
        copy.wait()


def shards(x_ckpt, bc_ckpt, step_sizes, decay_rate, skip_gain, grad_out):
    peers, blocks = lax.axis_size("tp"), lax.axis_size("seq")
    rows = x_ckpt.shape[0]
    head_count, tokens = step_sizes.shape
    width = grad_out.shape[1]
    state = bc_ckpt.shape[2]
    lanes = 128
    chunks = width // lanes
    head_width = width // head_count
    groups = chunks // 2 if chunks % 2 == 0 else chunks
    wide = lambda dtype, size: pltpu.VMEM((chunks, size, lanes), dtype)
    dma = lambda n: pltpu.SemaphoreType.DMA((n,))
    vmem = pl.BlockSpec(memory_space=pltpu.VMEM)
    hbm = pl.BlockSpec(memory_space=pl.ANY)
    heads = pltpu.VMEM((HEAD_PAD, tokens), F32)
    outs = (
        ((tokens, width), BF16),
        ((2, rows, state), F32),
        ((head_count, tokens), F32),
    )
    grads = pl.pallas_call(
        partial(kernel, peers, blocks, head_width),
        out_shape=tuple(pltpu.VMEM(shape, dtype) for shape, dtype in outs),
        in_specs=[hbm] * 6,
        out_specs=(vmem, vmem, vmem),
        scratch_shapes=[
            pltpu.VMEM(x_ckpt.shape, BF16),
            pltpu.VMEM((tokens, width), BF16),
            pltpu.VMEM((head_count, tokens), F32),
            pltpu.VMEM((peers, rows, width), BF16),
            pltpu.VMEM((peers, 2, rows, state), BF16),
            pltpu.VMEM((2, peers, rows, state), F32),
            *[wide(F32, state)] * 5,
            *[wide(BF16, state + TOP_ROWS)] * 4,
            pltpu.VMEM((peers, rows, width), BF16),
            pltpu.VMEM((peers, rows, state), BF16),
            pltpu.VMEM((head_count, tokens), F32),
            pltpu.VMEM((tokens, width), BF16),
            pltpu.VMEM((peers, rows, state), BF16),
            pltpu.VMEM((head_count, tokens), F32),
            pltpu.VMEM((2, HEAD_PAD, tokens), F32),
            pltpu.VMEM((2, chunks, tokens, lanes), F32),
            pltpu.VMEM((2, state, tokens), BF16),
            *[wide(BF16, tokens)] * 6,
            *[wide(F32, tokens)] * 2,
            wide(F32, 8),
            heads, heads, heads, heads,
            pltpu.VMEM((2, tokens, state), F32),
            heads, heads,
            pltpu.VMEM((4, tokens, tokens), BF16),
            pltpu.VMEM((2, tokens, state), BF16),
            pltpu.VMEM((2, state, tokens), BF16),
            pltpu.SMEM((head_count,), F32), pltpu.SMEM((head_count,), F32),
            dma(7), dma(12), dma(groups), dma(1), dma(chunks), dma(chunks), dma(2), dma(5),
        ],
        compiler_params=pltpu.CompilerParams(collective_id=0, has_side_effects=True),
    )(x_ckpt, bc_ckpt, step_sizes, decay_rate, skip_gain, grad_out)
    return pl.pallas_call(
        store,
        out_shape=tuple(jax.ShapeDtypeStruct(shape, dtype) for shape, dtype in outs),
        in_specs=[vmem] * 3,
        out_specs=(hbm,) * 3,
        scratch_shapes=[dma(3)],
    )(*[pltpu.with_memory_space_constraint(grad, pltpu.VMEM) for grad in grads])


def solution(mesh):
    return jax.shard_map(
        shards,
        mesh=mesh,
        in_specs=(
            P(("dp", "seq", "tp"), None),
            P(None, ("dp", "seq", "tp"), None),
            P("tp", ("dp", "seq")),
            P("tp"),
            P("tp"),
            P(("dp", "seq"), "tp"),
        ),
        out_specs=(
            P(("dp", "seq"), "tp"),
            P(None, ("dp", "seq", "tp"), None),
            P("tp", ("dp", "seq")),
        ),
        check_vma=False,
    )
```

```python
import math
from functools import partial

import jax
import jax.numpy as jnp
from jax import lax
from jax.experimental import pallas as pl
from jax.experimental.pallas import tpu as pltpu
from jax.sharding import PartitionSpec as P

MESH = pl.DeviceIdType.MESH
F32 = jnp.float32
BF16 = jnp.bfloat16
HEAD_PAD = 32
SKEW = 4
FOLLOW_FORWARD = 5
FOLLOW_BACK = 4
FIRST_BACK = 3
WORK_EVERY = 30
DIRECT = 2
SPAN = 125.0
TOP_ROWS = 8

NN = (((1,), (0,)), ((), ()))
NT = (((1,), (1,)), ((), ()))


def dot(a, b, dims=NN):
    return lax.dot_general(a, b, dims, preferred_element_type=F32)


def exact(a, b):
    return lax.dot_general(
        a, b, NN, precision=lax.Precision.HIGHEST, preferred_element_type=F32
    )


def split(v):
    high = v.astype(BF16)
    return high, (v - high.astype(F32)).astype(BF16)


def joined(a, b, dims=NN):
    return dot(jnp.concatenate(a, axis=1), jnp.concatenate(b, axis=dims[0][1][0]), dims)


def dot2(a, b, dims=NN):
    return joined((a, a), b, dims)


def dot2l(a, b, dims=NN):
    return joined(a, (b, b), dims)


def dot3(a, b, dims=NN):
    return joined((a[0], a[0], a[1]), (b[0], b[1], b[0]), dims)


def encode(v):
    top = jnp.max(jnp.abs(v), axis=0, keepdims=True)
    top = jnp.maximum(top, 1e-30).astype(BF16)
    code = jnp.exp2(v * (SPAN / top.astype(F32))).astype(BF16)
    return jnp.concatenate([code, jnp.broadcast_to(top, (TOP_ROWS, v.shape[1]))], axis=0)


def decode(message):
    size = message.shape[0] - TOP_ROWS
    top = message[size : size + 1].astype(F32)
    return jnp.log(message[0:size].astype(F32)) * (top * (1.0 / (SPAN * math.log(2.0))))


def kernel(
    peers, blocks, head_width,
    x_ref, bc_ref, step_ref, rate_ref, gain_ref, dy_ref,
    gx_ref, gbc_ref, gstep_ref,
    x_in, dy_in, step_in, xr, bcr, rs,
    state_in, state_out, pull_in, fresh, pulled,
    code_fo, code_fi, code_bo, code_bi,
    near_x, near_b, near_step, next_dy, next_c, next_step, pads, weights, sides,
    xs_h, xs_l, ys_h, ys_l, xc, dyc, ec, ed, gain_row,
    stp, rates, gains, cums, bc_acc, dcum_acc, dir_acc, sm, bcm, turned,
    rate_sm, gain_sm, own_sem, send_sem, recv_x, recv_b, recv_f, recv_g, recv_r, recv_n,
):
    me = lax.axis_index("tp")
    block = lax.axis_index("seq")
    head_count, tokens = step_ref.shape
    width = dy_ref.shape[1]
    rows = x_ref.shape[0]
    chunks, _, lanes = xc.shape
    chunk_heads = lanes // head_width
    groups = recv_x.shape[0]
    group_lanes = width // groups
    group_chunks = chunks // groups

    has_prev = block > 0
    has_next = block < blocks - 1

    mirror = peers - 1 - me
    if peers % 2 == 0:
        partners = [mirror]
        for i in range(2, peers, 2):
            partners += [lax.rem(me + i, peers), lax.rem(mirror + i, peers)]
    else:
        partners = [lax.rem(me + d, peers) for d in range(1, peers)]

    barrier = pltpu.get_barrier_semaphore()
    for peer in partners:
        pl.semaphore_signal(barrier, inc=1, device_id={"tp": peer}, device_id_type=MESH)

    def greet(there, exists, wide):
        @pl.when(jnp.logical_and(exists, wide))
        def _():
            for peer in range(peers):
                pl.semaphore_signal(
                    barrier, inc=1, device_id={"seq": there, "tp": peer}, device_id_type=MESH
                )

        @pl.when(jnp.logical_and(exists, jnp.logical_not(wide)))
        def _():
            pl.semaphore_signal(barrier, inc=1, device_id={"seq": there}, device_id_type=MESH)

        return jnp.where(exists, jnp.where(wide, peers, 1), 0)

    greeted = greet(block - 1, has_prev, jnp.logical_or(block == 1, block == blocks - 1))
    greeted += greet(block + 1, has_next, jnp.logical_or(block == 0, block == blocks - 2))

    own_bc = pltpu.make_async_copy(bc_ref, bcr.at[me], own_sem.at[0])
    load_x = pltpu.make_async_copy(x_ref, x_in, own_sem.at[1])
    own_x = pltpu.make_async_copy(
        x_ref.at[:, pl.ds(pl.multiple_of(me * width, 128), width)], xr.at[me], own_sem.at[2]
    )
    load_step = pltpu.make_async_copy(step_ref, step_in, own_sem.at[3])
    load_dy = pltpu.make_async_copy(dy_ref, dy_in, own_sem.at[4])
    load_rate = pltpu.make_async_copy(rate_ref, rate_sm, own_sem.at[5])
    load_gain = pltpu.make_async_copy(gain_ref, gain_sm, own_sem.at[6])
    own_bc.start()
    load_x.start()
    load_step.start()
    load_dy.start()
    own_x.start()
    load_rate.start()
    load_gain.start()

    def bc_copy(peer, slot):
        return pltpu.make_async_remote_copy(
            src_ref=bcr.at[me], dst_ref=bcr.at[slot],
            send_sem=send_sem.at[0], recv_sem=recv_b.at[0],
            device_id={"tp": peer}, device_id_type=MESH,
        )

    def x_copy(peer, slot, g):
        start = pl.multiple_of(peer * width + g * group_lanes, 128)
        return pltpu.make_async_remote_copy(
            src_ref=x_in.at[:, pl.ds(start, group_lanes)],
            dst_ref=xr.at[slot, :, pl.ds(g * group_lanes, group_lanes)],
            send_sem=send_sem.at[1], recv_sem=recv_x.at[g],
            device_id={"tp": peer}, device_id_type=MESH,
        )

    own_bc.wait()
    load_step.wait()
    pl.semaphore_wait(barrier, peers - 1 + greeted)

    def lend(source, target, slot, sem, there):
        return pltpu.make_async_remote_copy(
            src_ref=source, dst_ref=target, send_sem=send_sem.at[slot], recv_sem=sem,
            device_id={"seq": there}, device_id_type=MESH,
        )

    def lend_row(q, target, slot, sem, peer, there):
        return pltpu.make_async_remote_copy(
            src_ref=bcr.at[me, q], dst_ref=target.at[me],
            send_sem=send_sem.at[slot], recv_sem=sem,
            device_id={"seq": there, "tp": peer}, device_id_type=MESH,
        )

    @pl.when(block == 0)
    def _():
        lend(step_in, near_step, 9, recv_n.at[2], block + 1).start()
        for peer in (*partners, me):
            lend_row(0, near_b, 6, recv_n.at[0], peer, block + 1).start()

    @pl.when(block == blocks - 1)
    def _():
        lend(step_in, next_step, 10, recv_n.at[3], block - 1).start()
        for peer in (*partners, me):
            lend_row(1, next_c, 11, recv_n.at[1], peer, block - 1).start()

    for peer in partners:
        bc_copy(peer, me).start()

    direct = min(DIRECT, groups)

    def lend_x(c, slot):
        part = (slot, slice(None), pl.ds(c * lanes, lanes))
        return lend(xr.at[part], near_x.at[part], 7, recv_f.at[c], block + 1)

    def lend_own_x():
        part = (me, slice(None), pl.ds(direct * group_lanes, width - direct * group_lanes))
        return lend(xr.at[part], near_x.at[part], 7, recv_n.at[4], block + 1)

    def lend_direct(c, peer):
        start = pl.multiple_of(peer * width + c * lanes, 128)
        return pltpu.make_async_remote_copy(
            src_ref=x_in.at[:, pl.ds(start, lanes)],
            dst_ref=near_x.at[me, :, pl.ds(c * lanes, lanes)],
            send_sem=send_sem.at[7], recv_sem=recv_f.at[c],
            device_id={"seq": block + 1, "tp": peer}, device_id_type=MESH,
        )

    def lend_dy(c):
        part = (slice(None), pl.ds(c * lanes, lanes))
        return lend(dy_in.at[part], next_dy.at[part], 8, recv_g.at[c], block - 1)

    load_dy.wait()

    @pl.when(block == blocks - 1)
    def _():
        for c in range(chunks):
            lend_dy(c).start()

    load_x.wait()
    own_x.wait()
    for g in range(groups):
        if g < direct:
            @pl.when(block == 0)
            def _():
                for c in range(g * group_chunks, (g + 1) * group_chunks):
                    for peer in (*partners, me):
                        lend_direct(c, peer).start()

        if g == direct:
            @pl.when(block == 0)
            def _():
                lend_own_x().start()

        for peer in partners:
            x_copy(peer, me, g).start()

    load_rate.wait()
    load_gain.wait()
    stp[...] = jnp.zeros_like(stp)
    stp[0:head_count] = step_in[...]
    rates[...] = jnp.zeros_like(rates)
    gains[...] = jnp.zeros_like(gains)
    for h in range(head_count):
        rates[h : h + 1] = jnp.full((1, tokens), rate_sm[h], F32)
        gains[h : h + 1] = jnp.full((1, tokens), gain_sm[h], F32)
    row = lax.broadcasted_iota(jnp.int32, (tokens, tokens), 0)
    col = lax.broadcasted_iota(jnp.int32, (tokens, tokens), 1)
    upto = row <= col
    cum = exact(-rates[...] * stp[...], jnp.where(upto, 1.0, 0.0).astype(F32))
    cums[...] = cum
    stacked = jnp.concatenate(
        [jnp.exp(cum), jnp.exp(-cum) * stp[...], gains[...], jnp.zeros_like(cum)], axis=0
    )
    table = split(stacked.T)
    pick_row = lax.broadcasted_iota(jnp.int32, (4 * HEAD_PAD, lanes), 0)
    pick_head = lax.broadcasted_iota(jnp.int32, (4 * HEAD_PAD, lanes), 1) // head_width

    def spread(c, q):
        hit = pick_row == (q * HEAD_PAD + c * chunk_heads) + pick_head
        return jnp.where(hit, 1.0, 0.0).astype(BF16)

    for c in range(chunks):
        grown = dot2l(table, spread(c, 0))
        ec[c] = grown
        ed[c] = dot2l(table, spread(c, 1))
        gain_row[c] = dot2l((table[0][0:16], table[1][0:16]), spread(c, 2))[0:8]
        dy = dy_in[:, c * lanes : (c + 1) * lanes]
        dyc[c] = dy
        high, low = split(grown * dy.astype(F32))
        ys_h[c] = high
        ys_l[c] = low

    def forward_copy(c):
        return pltpu.make_async_remote_copy(
            src_ref=code_fo.at[c], dst_ref=code_fi.at[c],
            send_sem=send_sem.at[2], recv_sem=recv_f.at[c],
            device_id={"seq": block + 1}, device_id_type=MESH,
        )

    def backward_copy(c):
        return pltpu.make_async_remote_copy(
            src_ref=code_bo.at[c], dst_ref=code_bi.at[c],
            send_sem=send_sem.at[3], recv_sem=recv_g.at[c],
            device_id={"seq": block - 1}, device_id_type=MESH,
        )

    def landing(ref, sem, slot):
        return pltpu.make_async_remote_copy(
            src_ref=ref, dst_ref=ref, send_sem=send_sem.at[slot], recv_sem=sem,
            device_id={"tp": lax.rem(me + 1, peers)}, device_id_type=MESH,
        )

    def send_forward(c, value):
        code_fo[c] = encode(value)
        forward_copy(c).start()

    def send_backward(c, value):
        code_bo[c] = encode(value)
        backward_copy(c).start()

    def total_decay(c):
        return ec[c, tokens - 1 : tokens, :]

    def borrow(k, steps, weigh):
        landing(steps, recv_n.at[2 + k], 0).wait_recv()
        pads[k] = jnp.zeros_like(pads[k])
        pads[k, 0:head_count] = steps[...]
        cum = exact(-rates[...] * pads[k], jnp.where(upto, 1.0, 0.0).astype(F32))
        filler = jnp.zeros((3 * HEAD_PAD, tokens), F32)
        table = split(jnp.concatenate([weigh(cum, pads[k]), filler], axis=0).T)
        for c in range(chunks):
            weights[k, c] = dot2l(table, spread(c, 0))

    def borrow_side(k, side):
        landing(side, recv_n.at[k], 0).wait_recv()
        sides[k] = side[...].reshape(tokens, -1).astype(F32).T.astype(BF16)

    def gather_bc():
        landing(bcr.at[pl.ds(0, peers - 1)], recv_b.at[0], 0).wait_recv()
        proj_b = bcr[:, 0].reshape(tokens, -1)
        proj_c = bcr[:, 1].reshape(tokens, -1)
        bcm[0] = proj_b
        bcm[1] = proj_c
        turned[0] = proj_b.astype(F32).T.astype(BF16)
        turned[1] = proj_c.astype(F32).T.astype(BF16)
        scores_t = jnp.where(upto, dot(proj_b, proj_c, NT), 0.0)
        sm[0], sm[1] = split(scores_t)
        sm[2], sm[3] = split(scores_t.T)

    def pull_all():
        for c in range(chunks):
            pulled[c] = dot2(turned[1], (ys_h[c], ys_l[c]))

    def take_x(g):
        group = xr.at[pl.ds(0, peers - 1), :, pl.ds(g * group_lanes, group_lanes)]
        landing(group, recv_x.at[g], 1).wait_recv()
        if g >= direct:
            @pl.when(block == 0)
            def _():
                for c in range(g * group_chunks, (g + 1) * group_chunks):
                    for peer in partners:
                        lend_x(c, peer).start()

        for c in range(g * group_chunks, (g + 1) * group_chunks):
            x = xr[:, :, c * lanes : (c + 1) * lanes].reshape(tokens, lanes)
            xc[c] = x
            pair = split(ed[c] * x.astype(F32))
            xs_h[c] = pair[0]
            xs_l[c] = pair[1]
            fresh[c] = dot2(turned[0], pair)

    @pl.when(jnp.logical_not(has_next))
    def _():
        pull_in[...] = jnp.zeros_like(pull_in)

    dcum_acc[...] = jnp.zeros_like(dcum_acc)
    dir_acc[...] = jnp.zeros_like(dir_acc)

    def finish_inner():
        inner = jnp.zeros((tokens, tokens), F32)
        for c in range(chunks):
            inner += dot3((xs_h[c], xs_l[c]), (ys_h[c], ys_l[c]), NT)
        inner = jnp.where(upto, inner, 0.0)
        bc_acc[0] += dot2l(split(inner), bcm[1])
        bc_acc[1] += dot2l(split(inner.T), bcm[0])

    bc_acc[...] = jnp.zeros_like(bc_acc)

    def sum_copy(q, peer, slot):
        return pltpu.make_async_remote_copy(
            src_ref=bc_acc.at[q, pl.ds(pl.multiple_of(peer * rows, 8), rows)],
            dst_ref=rs.at[q, slot],
            send_sem=send_sem.at[4 + q], recv_sem=recv_r.at[q],
            device_id={"tp": peer}, device_id_type=MESH,
        )

    def send_sums(q):
        for peer in partners:
            sum_copy(q, peer, me).start()

    def selector(c):
        head = lax.broadcasted_iota(jnp.int32, (HEAD_PAD, lanes), 0)
        of = lax.broadcasted_iota(jnp.int32, (HEAD_PAD, lanes), 1) // head_width
        return jnp.where(head == c * chunk_heads + of, 1.0, 0.0).astype(BF16)

    def rebuilt(k, c, values):
        return dot2(sides[k], split(weights[k, c] * values.astype(F32)))

    def part_of(c):
        if isinstance(c, int):
            return pl.ds(c * lanes, lanes)
        return pl.ds(pl.multiple_of(c * lanes, 128), lanes)

    def forward_input(kind, c):
        if kind == "raw":
            if c == direct * group_chunks:
                rest = width - c * lanes
                landing(near_x.at[0, :, pl.ds(0, rest)], recv_n.at[4], 0).wait_recv()
            count = peers if c < direct * group_chunks else peers - 1
            part = near_x.at[pl.ds(0, count), :, pl.ds(0, lanes)]
            landing(part, recv_f.at[c], 0).wait_recv()
            entering = rebuilt(0, c, near_x[:, :, part_of(c)].reshape(tokens, lanes))
        else:
            forward_copy(c).wait_recv()
            entering = decode(code_fi[c])
        state_in[c] = entering
        return entering

    def backward_input(kind, c):
        if kind == "raw":
            landing(next_dy.at[:, pl.ds(0, lanes)], recv_g.at[c], 0).wait_recv()
            arriving = rebuilt(1, c, next_dy[:, part_of(c)])
        else:
            backward_copy(c).wait_recv()
            arriving = decode(code_bi[c])
        pull_in[c] = arriving
        return arriving

    def forward_link(kind, sends, c):
        if kind == "none":
            state_out[c] = total_decay(c) * fresh[c]
            return

        leaving = total_decay(c) * (forward_input(kind, c) + fresh[c])
        state_out[c] = leaving
        if sends:
            send_forward(c, leaving)

    def backward_link(kind, sends, c):
        if kind == "none":
            return
        arriving = backward_input(kind, c)
        if sends:
            send_backward(c, total_decay(c) * arriving + pulled[c])

    def forward_sum(kind, c):
        if kind != "none":
            bc_acc[1] += dot3((ys_h[c], ys_l[c]), split(state_in[c]), NT)

    def backward_sum(kind, c):
        if kind != "none":
            leaving = split(total_decay(c) * pull_in[c])
            bc_acc[0] += dot3((xs_h[c], xs_l[c]), leaving, NT)

    def forward_work(kind, c):
        left, right = (sm[2], sm[2], sm[3]), (xs_h[c], xs_l[c], xs_h[c])
        if kind != "none":
            left, right = (*left, bcm[1], bcm[1]), (*right, *split(state_in[c]))
        z = joined(left, right)
        dcum_acc[...] += dot2(selector(c), split(dyc[c].astype(F32) * z), NT)

    def backward_work(kind, c):
        left, right = (sm[0], sm[0], sm[1]), (ys_h[c], ys_l[c], ys_h[c])
        if kind != "none":
            leaving = split(total_decay(c) * pull_in[c])
            left, right = (*left, bcm[0], bcm[0]), (*right, *leaving)
        a2 = joined(left, right)
        x = xc[c].astype(F32)
        gx = ed[c] * a2 + gain_row[c, 0:1, :] * dyc[c].astype(F32)
        gx_ref[:, part_of(c)] = gx.astype(BF16)
        dir_acc[...] += dot2(selector(c), split(x * a2), NT)

    def grouped(part, *fixed):
        def run(g):
            for i in range(group_chunks):
                part(*fixed, g * group_chunks + i)
        return run

    def loop(low, high, *parts):
        def body(k, carry):
            for part, shift in parts:
                part(k + shift)
            return carry

        if high > low:
            lax.fori_loop(low, high, body, 0)

    def edge_role(link, add, work, other_work, early, late, flat):
        def take(g):
            for i in range(group_chunks):
                link(g * group_chunks + i)
                add(g * group_chunks + i)

        finish_inner()
        send_sums(early)
        loop(0, groups, (other_work, 0))
        if flat:
            for g in range(groups - 1):
                take(g)
                work(g)
        else:
            loop(0, groups - 1, (take, 0), (work, 0))
        take(groups - 1)
        send_sums(late)
        work(groups - 1)

    def inner_role(lead, follow, behind, done):
        (link1, add1, work1), (link2, add2, work2) = lead, follow
        links, adds, works = (link1, link2), (add1, add2), (work1, work2)
        steps = [(0, c) for c in range(chunks)]
        for c in reversed(range(chunks)):
            steps.insert(min(chunks, behind + 3 * c // 2 + 1), (1, c))
        ready = [(0, c) for c in range(group_chunks - 1, done, group_chunks)]
        steps = [step for step in steps if step not in [(0, c) for c in range(done)]]

        def add_group(side, g):
            for c in range(g * group_chunks, (g + 1) * group_chunks):
                adds[side](c)

        for at, (side, c) in enumerate(steps):
            links[side](c)
            if c % group_chunks == group_chunks - 1:
                ready.append((side, c))
            leading = any(other == 0 for other, _ in steps[at + 1 :])
            if ready and (not leading or at % WORK_EVERY == WORK_EVERY - 1):
                other, last = ready.pop(0)
                add_group(other, last // group_chunks)
                works[other](last // group_chunks)
        for side, last in ready:
            add_group(side, last // group_chunks)
        finish_inner()
        send_sums(0)
        send_sums(1)
        for side, last in ready:
            works[side](last // group_chunks)

    def between(s, carry):
        cf = s - SKEW * (block - 1)
        cb = s - SKEW * (blocks - 2 - block)

        @pl.when(jnp.logical_and(cf >= 0, cf < chunks))
        def _():
            forward_link("code", True, cf)
            forward_sum("code", cf)
            forward_work("code", cf)

        @pl.when(jnp.logical_and(cb >= 0, cb < chunks))
        def _():
            backward_link("code", True, cb)
            backward_sum("code", cb)
            backward_work("code", cb)

        return carry

    special = sorted({0, 1, blocks - 2, blocks - 1})
    for b in special:
        @pl.when(block == b)
        def _():
            forward = "none" if b == 0 else "raw" if b == 1 else "code"
            backward = "none" if b == blocks - 1 else "raw" if b == blocks - 2 else "code"
            sends = forward != "none" and backward != "none"
            ahead = (
                partial(forward_link, forward, sends),
                partial(forward_sum, forward), grouped(forward_work, forward),
            )
            behind = (
                partial(backward_link, backward, sends),
                partial(backward_sum, backward), grouped(backward_work, backward),
            )
            lag = (blocks - 2 - b) - (b - 1)
            if forward == "raw":
                borrow(
                    0, near_step,
                    lambda cum, steps: jnp.exp(cum[:, tokens - 1 : tokens] - cum) * steps,
                )
            if backward == "raw":
                borrow(1, next_step, lambda cum, steps: jnp.exp(cum))
            gather_bc()
            if sends:
                pull_all()
            if forward == "raw":
                borrow_side(0, near_b)
            if backward == "raw":
                borrow_side(1, next_c)
            done = 0
            if sends and lag < 0:
                done = min(FIRST_BACK, groups) * group_chunks
                for c in range(done):
                    behind[0](c)
            for g in range(groups):
                take_x(g)
                if sends and lag > 0 and g < direct:
                    done = (g + 1) * group_chunks
                    for c in range(g * group_chunks, done):
                        ahead[0](c)
            if forward == "none":
                loop(0, groups, (grouped(ahead[0]), 0))
                edge_role(*behind, ahead[2], 1, 0, backward == "raw")
            elif backward == "none":
                edge_role(*ahead, behind[2], 0, 1, forward == "raw")
            elif lag < 0:
                inner_role(behind, ahead, FOLLOW_FORWARD - 3 * (lag + 1), done)
            else:
                inner_role(ahead, behind, FOLLOW_BACK + 3 * max(lag - 1, 0), done)

    if blocks > 4:
        @pl.when(jnp.logical_and(block > 1, block < blocks - 2))
        def _():
            gather_bc()
            pull_all()
            for g in range(groups):
                take_x(g)
            lax.fori_loop(0, chunks + SKEW * (blocks - 3), between, 0)
            finish_inner()
            send_sums(1)
            send_sums(0)

    edge = jnp.zeros((HEAD_PAD, 8), F32)
    for c in range(chunks):
        both = (pull_in[c] * state_out[c]).reshape(-1, 8, lanes).sum(axis=0)
        edge = edge + dot2(selector(c), split(both), NT)
    edge = jnp.sum(edge, axis=1, keepdims=True)
    growth = jnp.exp(-cums[...])
    dcum = jnp.exp(cums[...]) * dcum_acc[...] - growth * stp[...] * dir_acc[...]
    after = exact(dcum, jnp.where(row >= col, 1.0, 0.0).astype(F32)) + edge
    gstep = growth * dir_acc[...] - rates[...] * after
    gstep_ref[...] = gstep[0:head_count]

    for q in range(2):
        landing(rs.at[q, pl.ds(0, peers - 1)], recv_r.at[q], 4 + q).wait_recv()
        total = bc_acc[q, pl.ds(pl.multiple_of(me * rows, 8), rows)]
        for peer in partners:
            total = total + rs[q, peer]
        gbc_ref[q] = total

    landing(bcr.at[pl.ds(0, peers - 1)], recv_b.at[0], 0).wait_send()
    landing(xr.at[pl.ds(0, peers - 1)], recv_x.at[0], 1).wait_send()
    for q in range(2):
        landing(rs.at[q, pl.ds(0, peers - 1)], recv_r.at[q], 4 + q).wait_send()

    inner_block = jnp.logical_and(has_prev, has_next)

    @pl.when(inner_block)
    def _():
        landing(code_fo, recv_f.at[0], 2).wait_send()
        landing(code_bo, recv_g.at[0], 3).wait_send()

    @pl.when(block == 0)
    def _():
        landing(near_b, recv_n.at[0], 6).wait_send()
        landing(near_step, recv_n.at[2], 9).wait_send()
        landing(near_x, recv_f.at[0], 7).wait_send()

    @pl.when(block == blocks - 1)
    def _():
        landing(next_c, recv_n.at[1], 11).wait_send()
        landing(next_step, recv_n.at[3], 10).wait_send()
        landing(dy_in, recv_g.at[0], 8).wait_send()


def store(gx_ref, gbc_ref, gstep_ref, gx_out, gbc_out, gstep_out, sems):
    copies = [
        pltpu.make_async_copy(source, target, sems.at[k])
        for k, (source, target) in enumerate(
            ((gx_ref, gx_out), (gbc_ref, gbc_out), (gstep_ref, gstep_out))
        )
    ]
    for copy in copies:
        copy.start()
    for copy in copies:
        copy.wait()


def shards(x_ckpt, bc_ckpt, step_sizes, decay_rate, skip_gain, grad_out):
    peers, blocks = lax.axis_size("tp"), lax.axis_size("seq")
    rows = x_ckpt.shape[0]
    head_count, tokens = step_sizes.shape
    width = grad_out.shape[1]
    state = bc_ckpt.shape[2]
    lanes = 128
    chunks = width // lanes
    head_width = width // head_count
    groups = chunks // 2 if chunks % 2 == 0 else chunks
    wide = lambda dtype, size: pltpu.VMEM((chunks, size, lanes), dtype)
    dma = lambda n: pltpu.SemaphoreType.DMA((n,))
    vmem = pl.BlockSpec(memory_space=pltpu.VMEM)
    hbm = pl.BlockSpec(memory_space=pl.ANY)
    heads = pltpu.VMEM((HEAD_PAD, tokens), F32)
    outs = (
        ((tokens, width), BF16),
        ((2, rows, state), F32),
        ((head_count, tokens), F32),
    )
    grads = pl.pallas_call(
        partial(kernel, peers, blocks, head_width),
        out_shape=tuple(pltpu.VMEM(shape, dtype) for shape, dtype in outs),
        in_specs=[hbm] * 6,
        out_specs=(vmem, vmem, vmem),
        scratch_shapes=[
            pltpu.VMEM(x_ckpt.shape, BF16),
            pltpu.VMEM((tokens, width), BF16),
            pltpu.VMEM((head_count, tokens), F32),
            pltpu.VMEM((peers, rows, width), BF16),
            pltpu.VMEM((peers, 2, rows, state), BF16),
            pltpu.VMEM((2, peers, rows, state), F32),
            *[wide(F32, state)] * 5,
            *[wide(BF16, state + TOP_ROWS)] * 4,
            pltpu.VMEM((peers, rows, width), BF16),
            pltpu.VMEM((peers, rows, state), BF16),
            pltpu.VMEM((head_count, tokens), F32),
            pltpu.VMEM((tokens, width), BF16),
            pltpu.VMEM((peers, rows, state), BF16),
            pltpu.VMEM((head_count, tokens), F32),
            pltpu.VMEM((2, HEAD_PAD, tokens), F32),
            pltpu.VMEM((2, chunks, tokens, lanes), F32),
            pltpu.VMEM((2, state, tokens), BF16),
            *[wide(BF16, tokens)] * 6,
            *[wide(F32, tokens)] * 2,
            wide(F32, 8),
            heads, heads, heads, heads,
            pltpu.VMEM((2, tokens, state), F32),
            heads, heads,
            pltpu.VMEM((4, tokens, tokens), BF16),
            pltpu.VMEM((2, tokens, state), BF16),
            pltpu.VMEM((2, state, tokens), BF16),
            pltpu.SMEM((head_count,), F32), pltpu.SMEM((head_count,), F32),
            dma(7), dma(12), dma(groups), dma(1), dma(chunks), dma(chunks), dma(2), dma(5),
        ],
        compiler_params=pltpu.CompilerParams(collective_id=0, has_side_effects=True),
    )(x_ckpt, bc_ckpt, step_sizes, decay_rate, skip_gain, grad_out)
    return pl.pallas_call(
        store,
        out_shape=tuple(jax.ShapeDtypeStruct(shape, dtype) for shape, dtype in outs),
        in_specs=[vmem] * 3,
        out_specs=(hbm,) * 3,
        scratch_shapes=[dma(3)],
    )(*[pltpu.with_memory_space_constraint(grad, pltpu.VMEM) for grad in grads])


def solution(mesh):
    return jax.shard_map(
        shards,
        mesh=mesh,
        in_specs=(
            P(("dp", "seq", "tp"), None),
            P(None, ("dp", "seq", "tp"), None),
            P("tp", ("dp", "seq")),
            P("tp"),
            P("tp"),
            P(("dp", "seq"), "tp"),
        ),
        out_specs=(
            P(("dp", "seq"), "tp"),
            P(None, ("dp", "seq", "tp"), None),
            P("tp", ("dp", "seq")),
        ),
        check_vma=False,
    )
```
